512 devices in a mesh: dp: 8 (over y_hi, x), expert: 64 (over z, y_lo, core).
Axes of the slice: x: 4, y: 8 (y_hi: 2, y_lo: 4; y = y_hi * 4 + y_lo), z: 8, core: 2. Of those that a mesh axis runs over, the one named last changes fastest.
Arguments:
- tokens: bfloat16 [65536, 1024], P(('dp', 'expert')), may hold values from -6 to 6
- out_grad: bfloat16 [65536, 1024], P(('dp', 'expert')), may hold values from -6 to 6
- expert_ids: int32 [65536, 3], P(('dp', 'expert')), may hold values from 0 to 63, all different within a row; in each aligned block of 128 rows (0 to 127, 128 to 255, ...) at most 7 rows name the same one
- gate_probs: float32 [65536, 3], P(('dp', 'expert')), may hold values from 0.1 to 0.6
- saved_pre: bfloat16 [8, 64, 448, 1536], P('dp', 'expert'), may hold values from -6 to 6
- gate_weight: bfloat16 [64, 1024, 768], P('expert', 'dp'), may hold values from -0.1875 to 0.1875
- up_weight: bfloat16 [64, 1024, 768], P('expert', 'dp'), may hold values from -0.1875 to 0.1875
- down_weight: bfloat16 [64, 1024, 768], P('expert', 'dp'), may hold values from -0.21875 to 0.21875
- basis: bfloat16 [64, 1024, 256], P('expert', 'dp'), may hold values from -0.1875 to 0.1875
Outputs:
- in_grad: bfloat16 [65536, 1024], P(('dp', 'expert'))
- proj_grads: float32 [64, 3, 256, 768], P('expert', None, 'dp')
The draws below stay inside these ranges and needn't reach their ends.
Inputs may be any that keep to these rules, and one draw needn't show every extreme that they name: `expert_ids`: each token names 3 different experts. The rows of one device name one expert at most 7 times, and on some devices some expert exactly 7 times.
All inputs are finite; a program needn't handle non-finite values.
Results may differ from the reference program's by a relative error of at most 0.0091.
Values may be sent and summed in bfloat16 or wider, within the bound.
No kernel may reach another device: no remote copies, remote signals or barrier semaphores. Data moves between devices by JAX's collectives and lax.ppermute only.
A program may use at most 64 MiB of HBM per device.

```python
import math
import jax
import jax.numpy as jnp
import numpy as np
from jax import lax

D = 1024
FF = 768
RANK = 256
TOPK = 3
TOK_DEV = 128
EXPERTS = 64
CAP = 7
SLOTS = 448
TOKENS = 65536
N_DP = 8
N_EXPERT = 64


def block_scale(stream_key, extent, cuts, smallest, largest):
    loudness, own = 1.0, jax.random.fold_in(stream_key, 6)
    for dim, blocks in cuts:
        draws = jnp.exp(jax.random.uniform(jax.random.fold_in(own, dim), (blocks,), jnp.float32, smallest / len(cuts), largest / len(cuts)))
        loudness = loudness * jnp.repeat(draws, extent[dim] // blocks).reshape([-1 if axis == dim else 1 for axis in range(len(extent))])
    return loudness


def assign_block(own_key, own, number, rows, amount, top, reach, slope):
    order = jax.random.permutation(own_key, amount)
    packed, ordinary = load_shares(amount, rows * top, reach, slope, True), load_shares(amount, rows * top, reach, slope, False)
    places = jnp.arange(amount)

    def named(sizes, rotation):
        used = int((sizes > 0).sum())
        fixed = max(1, used // 4)
        moved = fixed + (places - fixed + rotation * (used - fixed)) % max(1, amount - fixed)
        return jnp.zeros((amount,), jnp.int32).at[order[jnp.where(places < fixed, places, moved)]].set(jnp.asarray(sizes, jnp.int32))

    sizes = jnp.where(number % 4 == 0, named(packed, number // 4), named(ordinary, number - number // 4 - 1))
    mixed = jax.random.permutation(jax.random.fold_in(own, 3), amount)
    source_of, sink = mixed[0:amount // 2 * 2:2], mixed[1:amount // 2 * 2:2]
    margin = jnp.minimum(sizes[source_of] - 1, reach - sizes[sink]) // 2
    margin = jnp.where((source_of == order[0]) | (sink == order[0]) | (sizes[sink] == 0), 0, jnp.maximum(margin, 0))
    moved = jax.random.randint(jax.random.fold_in(own, 4), (amount // 2,), 0, 1 << 20) % (margin + 1)
    sizes = sizes.at[source_of].add(-moved).at[sink].add(moved)
    members = jnp.searchsorted(jnp.cumsum(sizes), jnp.arange(rows * top), side="right").astype(jnp.int32)
    grid = members.reshape(top, rows).T
    grid = grid[jax.random.permutation(jax.random.fold_in(own, 1), rows)]
    rotation = jax.random.randint(jax.random.fold_in(own, 2), (rows, 1), 0, top)
    return jnp.take_along_axis(grid, (jnp.arange(top)[None, :] + rotation) % top, axis=1)


def load_shares(count, total, limit, skew, full):
    portions = [(1 << 20) // math.isqrt(grade ** skew) + 1 for grade in range(1, count + 1)]
    largest = limit if full else min(limit, max(-(-total // count), total * portions[0] // sum(portions)))
    least = 1 if total - largest >= count - 1 else 0
    counts, surplus = [largest] + [least] * (count - 1), total - largest - least * (count - 1)
    while surplus > 0:
        candidates = [i for i in range(1, count) if counts[i] < largest] or [i for i in range(1, count) if counts[i] < limit]
        mass, budget = sum([portions[i] for i in candidates]), surplus
        for i in candidates:
            addition = min(limit - counts[i], max(1, budget * portions[i] // mass), surplus)
            counts[i] = counts[i] + addition
            surplus = surplus - addition
    return np.array(counts)


def scatter_about(rng, dims, width, reach, shards=(), kind=jnp.bfloat16):
    entries = width * jax.random.normal(rng, dims, jnp.float32)
    if shards:
        entries = entries * block_scale(rng, dims, shards, -0.22, 0.18)
    return jnp.clip(entries, -reach, reach).astype(kind)


def setup_inputs(seed: int = 0) -> dict:
    arg_keys = jax.random.split(jax.random.key(seed), 10)
    tokens = scatter_about(arg_keys[0], (TOKENS, D), 1.0, 6.0, ((0, 512),))
    out_grad = scatter_about(arg_keys[1], (TOKENS, D), 1.0, 6.0, ((0, 512),))
    expert_ids_keys = jax.random.split(jax.random.fold_in(arg_keys[2], 1), TOKENS // TOK_DEV)
    expert_ids_turns = jax.random.permutation(jax.random.fold_in(arg_keys[2], 3), TOKENS // TOK_DEV)
    expert_ids = jax.vmap(lambda own, number: assign_block(jax.random.fold_in(arg_keys[2], 2), own, number, TOK_DEV, EXPERTS, TOPK, CAP, 2))(expert_ids_keys, expert_ids_turns).reshape((TOKENS, TOPK))
    gate_probs = jnp.clip(0.1 + 0.5 * jax.random.uniform(arg_keys[3], (TOKENS, TOPK), jnp.float32) ** block_scale(arg_keys[3], (TOKENS, TOPK), ((0, 512),), -0.2, 0.2), 0.1, 0.6)
    saved_pre = scatter_about(arg_keys[4], (N_DP, EXPERTS, SLOTS, 2 * FF), 1.5, 6.0, ((0, 8), (1, 64)))
    gate_weight = scatter_about(arg_keys[5], (EXPERTS, D, FF), D ** -0.5, 0.1875, ((0, 64), (1, 8)))
    up_weight = scatter_about(arg_keys[6], (EXPERTS, D, FF), D ** -0.5, 0.1875, ((0, 64), (1, 8)))
    down_weight = scatter_about(arg_keys[7], (EXPERTS, D, FF), FF ** -0.5, 0.21875, ((0, 64), (1, 8)))
    basis = scatter_about(arg_keys[8], (EXPERTS, D, RANK), D ** -0.5, 0.1875, ((0, 64), (1, 8)))
    return {"tokens": tokens, "out_grad": out_grad, "expert_ids": expert_ids, "gate_probs": gate_probs, "saved_pre": saved_pre, "gate_weight": gate_weight, "up_weight": up_weight, "down_weight": down_weight, "basis": basis}


def slot_tables(expert_ids):
    devices = N_DP * N_EXPERT
    ids = expert_ids.reshape(devices, TOK_DEV, TOPK)
    onehot = (ids[:, :, :, None] == jnp.arange(EXPERTS, dtype=jnp.int32)[None, None, None, :]).astype(jnp.int32)
    per_token = jnp.sum(onehot, axis=2)
    before = jnp.cumsum(per_token, axis=1) - per_token
    position = jnp.sum(onehot * before[:, :, None, :], axis=3)
    device = jnp.arange(devices, dtype=jnp.int32)[:, None, None]
    group = device // N_EXPERT
    source = device % N_EXPERT
    flat = (group * EXPERTS + ids) * SLOTS + source * CAP + position
    token_index = device * TOK_DEV + jnp.arange(TOK_DEV, dtype=jnp.int32)[None, :, None]
    token_index = jnp.broadcast_to(token_index, ids.shape)
    choice_index = jnp.broadcast_to(jnp.arange(TOPK, dtype=jnp.int32)[None, None, :], ids.shape)
    table_token = jnp.full((N_DP * EXPERTS * SLOTS,), -1, jnp.int32).at[flat.reshape(-1)].set(token_index.reshape(-1))
    table_choice = jnp.zeros((N_DP * EXPERTS * SLOTS,), jnp.int32).at[flat.reshape(-1)].set(choice_index.reshape(-1))
    return table_token.reshape(N_DP, EXPERTS, SLOTS), table_choice.reshape(N_DP, EXPERTS, SLOTS)


def reference(tokens, out_grad, expert_ids, gate_probs, saved_pre, gate_weight, up_weight, down_weight, basis):
    table_token, table_choice = slot_tables(expert_ids)

    def per_expert(accum, expert):
        w_gate = gate_weight[expert]
        w_up = up_weight[expert]
        w_down = down_weight[expert]
        w_basis = basis[expert]

        def per_group(carry, group):
            total, projected = carry
            taken = table_token[group, expert]
            chosen = table_choice[group, expert]
            filled = taken >= 0
            picked = jnp.maximum(taken, 0).astype(jnp.int32)
            x_rows = jnp.where(filled[:, None], tokens[picked], jnp.zeros((), jnp.bfloat16))
            weight_pick = gate_probs[picked, chosen]
            scaled = (out_grad[picked].astype(jnp.float32) * weight_pick[:, None]).astype(jnp.bfloat16)
            dy_rows = jnp.where(filled[:, None], scaled, jnp.zeros((), jnp.bfloat16))
            pre = saved_pre[group, expert].astype(jnp.float32)
            gate_pre = pre[:, :FF]
            up_pre = pre[:, FF:]
            hidden_grad = jnp.dot(dy_rows, w_down, preferred_element_type=jnp.float32)
            x_proj = jnp.dot(x_rows, w_basis, preferred_element_type=jnp.float32).astype(jnp.bfloat16)
            dy_proj = jnp.dot(dy_rows, w_basis, preferred_element_type=jnp.float32).astype(jnp.bfloat16)
            sig = jax.nn.sigmoid(gate_pre)
            hid = (gate_pre * sig * up_pre).astype(jnp.bfloat16)
            up_grad = (hidden_grad * gate_pre * sig).astype(jnp.bfloat16)
            gate_grad = (hidden_grad * up_pre * sig * (1.0 + gate_pre * (1.0 - sig))).astype(jnp.bfloat16)
            terms = jnp.stack([
                jnp.dot(x_proj.T, gate_grad, preferred_element_type=jnp.float32),
                jnp.dot(x_proj.T, up_grad, preferred_element_type=jnp.float32),
                jnp.dot(dy_proj.T, hid, preferred_element_type=jnp.float32)])
            row_grad = jnp.dot(gate_grad, w_gate.T, preferred_element_type=jnp.float32)
            row_grad = row_grad + jnp.dot(up_grad, w_up.T, preferred_element_type=jnp.float32)
            row_grad = row_grad.astype(jnp.bfloat16).astype(jnp.float32)
            row_grad = jnp.where(filled[:, None], row_grad, jnp.zeros((), jnp.float32))
            total = total.at[picked].add(row_grad)
            return (total, projected + terms), None

        start = (accum, jnp.zeros((3, RANK, FF), jnp.float32))
        (accum, projected), unused = lax.scan(per_group, start, jnp.arange(N_DP, dtype=jnp.int32))
        return accum, projected

    accum = jnp.zeros((TOKENS, D), jnp.float32)
    accum, proj_grads = lax.scan(per_expert, accum, jnp.arange(EXPERTS, dtype=jnp.int32))
    return accum.astype(jnp.bfloat16), proj_grads
```

```python
import functools

import jax
import jax.numpy as jnp
from jax import lax
from jax.experimental import pallas as pl
from jax.experimental.pallas import tpu as pltpu
from jax.sharding import Mesh
from jax.sharding import PartitionSpec as P


DP = ("dp_0", "dp_1")
DP_EXPERT = ("dp_0", "dp_1", "expert")
F32 = jnp.float32
BF16 = jnp.bfloat16
LANES = 128


def chunk_rows(start, slots, step):
    return pl.ds(start, slots, stride=step)


def pack_kernel(cap, ids_ref, probs_ref, tok_ref, grad_ref, out_ref, match_ref, wide_ref):
    slots, n_tok = match_ref.shape
    topk = ids_ref.shape[0]
    n_owner = slots // cap
    ids = ids_ref[...]
    probs = probs_ref[...]
    owner = lax.broadcasted_iota(jnp.int32, (n_owner, n_tok), 0)
    named = [owner == ids[k : k + 1, :] for k in range(topk)]
    per_owner = sum(n.astype(F32) for n in named)
    earlier = (
        lax.broadcasted_iota(jnp.int32, (n_tok, n_tok), 0)
        < lax.broadcasted_iota(jnp.int32, (n_tok, n_tok), 1)
    ).astype(F32)
    before = jnp.dot(per_owner.astype(BF16), earlier.astype(BF16), preferred_element_type=F32)
    slot = lax.broadcasted_iota(jnp.int32, (slots, n_tok), 0)
    match = jnp.zeros((slots, n_tok), F32)
    weight = jnp.zeros((slots, n_tok), F32)
    for k in range(topk):
        position = jnp.sum(jnp.where(named[k], before, 0.0), axis=0, keepdims=True)
        here = slot == ids[k : k + 1, :] * cap + position.astype(jnp.int32)
        match = match + here.astype(F32)
        weight = weight + jnp.where(here, probs[k : k + 1, :], 0.0)
    weight = jnp.sum(weight, axis=1, keepdims=True)
    match = match.astype(BF16)
    match_ref[...] = match
    n_chunk = tok_ref.shape[1] // LANES
    for half, src in enumerate((tok_ref, grad_ref)):
        for c in range(0, n_chunk, 2):
            rows = jnp.dot(
                match, src[:, c * LANES : (c + 2) * LANES], preferred_element_type=F32
            )
            if half:
                rows = rows * weight
            for i in range(2):
                wide_ref[chunk_rows(half * n_chunk + c + i, slots, 2 * n_chunk), :] = rows[
                    :, i * LANES : (i + 1) * LANES
                ]
    out_ref[...] = wide_ref[...].astype(BF16)


def pack(ids, probs, tokens, out_grad, n_owner, cap):
    n_tok, width = tokens.shape
    slots = n_owner * cap
    rows = slots * 2 * width // LANES
    return pl.pallas_call(
        functools.partial(pack_kernel, cap),
        out_shape=(
            jax.ShapeDtypeStruct((rows, LANES), BF16),
            jax.ShapeDtypeStruct((slots, n_tok), BF16),
        ),
        scratch_shapes=[pltpu.VMEM((rows, LANES), F32)],
        name="pack",
    )(ids, probs, tokens, out_grad)


def take_pair(wide_ref, first, second, slots, step):
    return jnp.concatenate(
        [
            wide_ref[chunk_rows(first, slots, step), :],
            wide_ref[chunk_rows(second, slots, step), :],
        ],
        axis=1,
    ).astype(BF16)


def piece_index(where_ref, k):
    high, low, n_low = where_ref[0], where_ref[1], 4
    column = lax.rem(low - k + n_low, n_low)
    return high * n_low + column, (1 - high) * n_low + column


def grads_kernel(n_piece, hidden, *refs):
    where_ref, got_ref, pre_ref = refs[:3]
    mine1, other1 = refs[3 : 3 + n_piece], refs[3 + n_piece : 3 + 2 * n_piece]
    at = 3 + 2 * n_piece
    mine2, other2 = refs[at : at + n_piece], refs[at + n_piece : at + 2 * n_piece]
    row_ref, both_ref, hid_ref, proj_ref, wide_ref, narrow_ref = refs[at + 2 * n_piece :]
    slots = pre_ref.shape[0]
    n_chunk = 2 * n_piece
    wide_ref[...] = got_ref[...].astype(F32)
    total = None
    for k in range(n_piece):
        first, second = piece_index(where_ref, k)
        left = take_pair(wide_ref, n_chunk + first, n_chunk + second, slots, 2 * n_chunk)
        right = jnp.concatenate([mine1[k][...], other1[k][...]], axis=0)
        part = jnp.dot(left, right, preferred_element_type=F32)
        total = part if total is None else total + part
    proj_ref[...] = total[:, hidden:].astype(BF16)
    grad = total[:, :hidden]
    gate = pre_ref[:, :hidden].astype(F32)
    up = pre_ref[:, hidden:].astype(F32)
    sig = jax.nn.sigmoid(gate)
    act = gate * sig
    hid_ref[...] = (act * up).astype(BF16)
    both_ref[:, hidden:] = (grad * act).astype(BF16)
    both_ref[:, :hidden] = (grad * up * sig * (1.0 + gate * (1.0 - sig))).astype(BF16)
    for k in range(n_piece):
        first, second = piece_index(where_ref, k)
        right = jnp.concatenate([mine2[k][...], other2[k][...]], axis=0)
        rows = lax.dot_general(
            both_ref[...], right, (((1,), (1,)), ((), ())), preferred_element_type=F32
        )
        narrow_ref[chunk_rows(first, slots, n_chunk), :] = rows[:, :LANES]
        narrow_ref[chunk_rows(second, slots, n_chunk), :] = rows[:, LANES:]
    row_ref[...] = narrow_ref[...].astype(BF16)


def vmem():
    return pl.BlockSpec(memory_space=pltpu.VMEM)


def grads(where, got, pre, mine1, other1, mine2, other2, hidden, width):
    slots = pre.shape[0]
    n_piece = len(mine1)
    rank = mine1[0].shape[1] - hidden
    n_in = 2 + 4 * n_piece
    return pl.pallas_call(
        functools.partial(grads_kernel, n_piece, hidden),
        in_specs=[pl.BlockSpec(memory_space=pltpu.SMEM)] + [vmem()] * n_in,
        out_shape=(
            jax.ShapeDtypeStruct((slots * width // LANES, LANES), BF16),
            jax.ShapeDtypeStruct((slots, 2 * hidden), BF16),
            jax.ShapeDtypeStruct((slots, hidden), BF16),
            jax.ShapeDtypeStruct((slots, rank), BF16),
        ),
        scratch_shapes=[
            pltpu.VMEM((2 * slots * width // LANES, LANES), F32),
            pltpu.VMEM((slots * width // LANES, LANES), F32),
        ],
        name="grads",
    )(where, got, pre, *mine1, *other1, *mine2, *other2)


def terms_kernel(n_piece, hidden, *refs):
    where_ref, got_ref, both_ref, hid_ref, proj_ref = refs[:5]
    mine1, other1 = refs[5 : 5 + n_piece], refs[5 + n_piece : 5 + 2 * n_piece]
    out_ref, wide_ref = refs[5 + 2 * n_piece :]
    slots = hid_ref.shape[0]
    n_chunk = 2 * n_piece
    wide_ref[...] = got_ref[...].astype(F32)
    total = None
    for k in range(n_piece):
        first, second = piece_index(where_ref, k)
        left = take_pair(wide_ref, first, second, slots, 2 * n_chunk)
        right = jnp.concatenate([mine1[k][:, hidden:], other1[k][:, hidden:]], axis=0)
        part = jnp.dot(left, right, preferred_element_type=F32)
        total = part if total is None else total + part
    x_proj = total.astype(BF16)
    by_rows = (((0,), (0,)), ((), ()))
    first_two = lax.dot_general(x_proj, both_ref[...], by_rows, preferred_element_type=F32)
    last = lax.dot_general(proj_ref[...], hid_ref[...], by_rows, preferred_element_type=F32)
    part = x_proj.shape[1] // n_chunk
    for n, term in enumerate((first_two[:, :hidden], first_two[:, hidden:], last)):
        term = term.astype(BF16)
        for d in range(n_chunk):
            out_ref[d % n_piece, d // n_piece, n] = term[d * part : (d + 1) * part]


def terms(where, got, both, hid, proj, mine1, other1):
    hidden = hid.shape[1]
    n_piece = len(mine1)
    part = proj.shape[1] // (2 * n_piece)
    return pl.pallas_call(
        functools.partial(terms_kernel, n_piece, hidden),
        in_specs=[pl.BlockSpec(memory_space=pltpu.SMEM)] + [vmem()] * (4 + 2 * n_piece),
        out_shape=jax.ShapeDtypeStruct((n_piece, 2, 3, part, hidden), BF16),
        scratch_shapes=[pltpu.VMEM(got.shape, F32)],
        name="terms",
    )(where, got, both, hid, proj, *mine1, *other1)


def combine_kernel(match_ref, got_ref, out_ref, wide_ref):
    slots = match_ref.shape[0]
    n_chunk = out_ref.shape[1] // LANES
    wide_ref[...] = got_ref[...].astype(F32)
    for c in range(0, n_chunk, 2):
        rows = take_pair(wide_ref, c, c + 1, slots, n_chunk)
        total = lax.dot_general(
            match_ref[...], rows, (((0,), (0,)), ((), ())), preferred_element_type=F32
        )
        out_ref[:, c * LANES : (c + 2) * LANES] = total.astype(BF16)


def combine(match, got, width):
    n_tok = match.shape[1]
    return pl.pallas_call(
        combine_kernel,
        out_shape=jax.ShapeDtypeStruct((n_tok, width), BF16),
        scratch_shapes=[pltpu.VMEM(got.shape, F32)],
        name="combine",
    )(match, got)


def swap(value):
    return lax.ppermute(value, "dp_0", [(0, 1), (1, 0)])


def shifted(value):
    size = lax.axis_size("dp_1")
    return [
        lax.ppermute(value, "dp_1", [(i, (i + k) % size) for i in range(size)])
        for k in range(1, size)
    ]


def exchange(value, n_owner):
    rows, lanes = value.shape
    out = lax.all_to_all(
        value.reshape(n_owner, rows // n_owner, lanes), "expert", 0, 0, tiled=True
    )
    return out.reshape(rows, lanes)


def body(
    tokens, out_grad, expert_ids, gate_probs, saved_pre, gate_weight, up_weight, down_weight, basis
):
    n_owner = lax.axis_size("expert")
    width = tokens.shape[1]
    slots = saved_pre.shape[2]
    cap = slots // n_owner
    hidden = gate_weight.shape[2]
    where = jnp.stack([lax.axis_index("dp_0"), lax.axis_index("dp_1")]).astype(jnp.int32)

    w1 = jnp.concatenate([down_weight[0], basis[0]], axis=1)
    far1 = swap(w1)
    sent, match = pack(expert_ids.T, gate_probs.T, tokens, out_grad, n_owner, cap)
    got = exchange(sent, n_owner)
    w2 = jnp.concatenate([gate_weight[0], up_weight[0]], axis=1)
    far2 = swap(w2)
    mine1 = [w1] + shifted(w1)
    mine2 = [w2] + shifted(w2)
    other1 = [far1] + shifted(far1)
    other2 = [far2] + shifted(far2)
    row_grad, both, hid, proj = grads(
        where, got, saved_pre[0, 0], mine1, other1, mine2, other2, hidden, width
    )
    back = exchange(row_grad, n_owner)
    parts = terms(where, got, both, hid, proj, mine1, other1)
    n_low, n_high, n_term, part, _ = parts.shape
    parts = parts.reshape(n_low, n_high * n_term * part, hidden)
    low = lax.axis_index("dp_1")
    summed = lax.dynamic_index_in_dim(parts, low, 0, keepdims=False).astype(F32)
    for k in range(1, n_low):
        out = lax.dynamic_index_in_dim(parts, lax.rem(low + k, n_low), 0, keepdims=False)
        out = lax.ppermute(out, "dp_1", [(i, (i + k) % n_low) for i in range(n_low)])
        summed = summed + out.astype(F32)
    summed = summed.reshape(n_high, n_term * part, hidden)
    high = lax.axis_index("dp_0")
    mine = jnp.where(high == 0, summed[0], summed[1])
    other = jnp.where(high == 0, summed[1], summed[0]).astype(BF16)
    other = swap(other)
    proj_grads = (mine + other.astype(F32)).reshape(1, n_term, part, hidden)
    in_grad = combine(match, back, width)
    return in_grad, proj_grads


def solution(mesh):
    finer = Mesh(mesh.devices.reshape(2, 4, mesh.shape["expert"]), DP_EXPERT)
    placed = (
        P(DP_EXPERT, None),
        P(DP_EXPERT, None),
        P(DP_EXPERT, None),
        P(DP_EXPERT, None),
        P(DP, "expert", None, None),
        P("expert", DP, None),
        P("expert", DP, None),
        P("expert", DP, None),
        P("expert", DP, None),
    )
    return jax.shard_map(
        body,
        mesh=finer,
        in_specs=placed,
        out_specs=(P(DP_EXPERT, None), P("expert", None, DP, None)),
        check_vma=False,
    )
```

```python
import functools

import jax
import jax.numpy as jnp
from jax import lax
from jax.experimental import pallas as pl
from jax.experimental.pallas import tpu as pltpu
from jax.sharding import Mesh
from jax.sharding import PartitionSpec as P


DP = ("dp_0", "dp_1")
DP_EXPERT = ("dp_0", "dp_1", "expert")
F32 = jnp.float32
BF16 = jnp.bfloat16
LANES = 128


def chunk_rows(start, slots, step):
    return pl.ds(start, slots, stride=step)


def pack_kernel(cap, ids_ref, probs_ref, tok_ref, grad_ref, out_ref, match_ref, wide_ref):
    slots, n_tok = match_ref.shape
    topk = ids_ref.shape[0]
    n_owner = slots // cap
    ids = ids_ref[...]
    probs = probs_ref[...]
    owner = lax.broadcasted_iota(jnp.int32, (n_owner, n_tok), 0)
    named = [owner == ids[k : k + 1, :] for k in range(topk)]
    per_owner = sum(n.astype(F32) for n in named)
    earlier = (
        lax.broadcasted_iota(jnp.int32, (n_tok, n_tok), 0)
        < lax.broadcasted_iota(jnp.int32, (n_tok, n_tok), 1)
    ).astype(F32)
    before = jnp.dot(per_owner.astype(BF16), earlier.astype(BF16), preferred_element_type=F32)
    slot = lax.broadcasted_iota(jnp.int32, (slots, n_tok), 0)
    match = jnp.zeros((slots, n_tok), F32)
    weight = jnp.zeros((slots, n_tok), F32)
    for k in range(topk):
        position = jnp.sum(jnp.where(named[k], before, 0.0), axis=0, keepdims=True)
        here = slot == ids[k : k + 1, :] * cap + position.astype(jnp.int32)
        match = match + here.astype(F32)
        weight = weight + jnp.where(here, probs[k : k + 1, :], 0.0)
    weight = jnp.sum(weight, axis=1, keepdims=True)
    match = match.astype(BF16)
    match_ref[...] = match
    n_chunk = tok_ref.shape[1] // LANES
    for half, src in enumerate((tok_ref, grad_ref)):
        for c in range(0, n_chunk, 2):
            rows = jnp.dot(
                match, src[:, c * LANES : (c + 2) * LANES], preferred_element_type=F32
            )
            if half:
                rows = rows * weight
            for i in range(2):
                wide_ref[chunk_rows(half * n_chunk + c + i, slots, 2 * n_chunk), :] = rows[
                    :, i * LANES : (i + 1) * LANES
                ]
    out_ref[...] = wide_ref[...].astype(BF16)


def pack(ids, probs, tokens, out_grad, n_owner, cap):
    n_tok, width = tokens.shape
    slots = n_owner * cap
    rows = slots * 2 * width // LANES
    return pl.pallas_call(
        functools.partial(pack_kernel, cap),
        out_shape=(
            jax.ShapeDtypeStruct((rows, LANES), BF16),
            jax.ShapeDtypeStruct((slots, n_tok), BF16),
        ),
        scratch_shapes=[pltpu.VMEM((rows, LANES), F32)],
        name="pack",
    )(ids, probs, tokens, out_grad)


def piece_rows(where_ref, k, other):
    high, low = where_ref[0], where_ref[1]
    row = jnp.bitwise_and(high + other, 1) * 4 + jnp.bitwise_and(low + 4 - k, 3)
    return pl.ds(pl.multiple_of(row * LANES, LANES), LANES)


def fetch_pieces(where_ref, pieces, columns, into, sems):
    copies = []
    for i, piece in enumerate(pieces):
        rows = piece_rows(where_ref, i // 2, i % 2)
        copy = pltpu.make_async_copy(piece.at[:, columns], into.at[rows, :], sems.at[i])
        copy.start()
        copies.append(copy)
    return copies


def spread(wide_ref, first, step, into):
    slots, width = into.shape
    for c in range(width // LANES):
        into[:, c * LANES : (c + 1) * LANES] = wide_ref[
            chunk_rows(first + c, slots, step), :
        ].astype(BF16)


def core_kernel(n_piece, hidden, *refs):
    where_ref, got_ref, pre_ref = refs[:3]
    pieces = refs[3 : 3 + n_piece]
    outs = refs[3 + n_piece : 3 + n_piece + 5]
    both_ref, part_refs = outs[0], outs[1:]
    got, pre, weights, wide, x_rows, dy_rows, term_ref, sems = refs[3 + n_piece + 5 :]
    width = weights.shape[0]
    n_chunk = width // LANES
    fetch_got = pltpu.make_async_copy(got_ref, got, sems.at[n_piece])
    fetch_got.start()
    copies = fetch_pieces(where_ref, pieces, pl.ds(0, weights.shape[1]), weights, sems)
    fetch_pre = pltpu.make_async_copy(pre_ref, pre, sems.at[n_piece + 1])
    fetch_pre.start()
    fetch_got.wait()
    wide[...] = got[...].astype(F32)
    spread(wide, n_chunk, 2 * n_chunk, dy_rows)
    spread(wide, 0, 2 * n_chunk, x_rows)
    for copy in copies:
        copy.wait()
    grad = jnp.dot(dy_rows[...], weights[:, :hidden], preferred_element_type=F32)
    dy_proj = jnp.dot(dy_rows[...], weights[:, hidden:], preferred_element_type=F32).astype(BF16)
    x_proj = jnp.dot(x_rows[...], weights[:, hidden:], preferred_element_type=F32).astype(BF16)
    fetch_pre.wait()
    gate = pre[:, :hidden].astype(F32)
    up = pre[:, hidden:].astype(F32)
    sig = jax.nn.sigmoid(gate)
    act = gate * sig
    hid = (act * up).astype(BF16)
    both_ref[:, hidden:] = (grad * act).astype(BF16)
    both_ref[:, :hidden] = (grad * up * sig * (1.0 + gate * (1.0 - sig))).astype(BF16)
    by_rows = (((0,), (0,)), ((), ()))
    term_ref[2] = lax.dot_general(dy_proj, hid, by_rows, preferred_element_type=F32)
    term_ref[0] = lax.dot_general(
        x_proj, both_ref[:, :hidden], by_rows, preferred_element_type=F32
    )
    term_ref[1] = lax.dot_general(
        x_proj, both_ref[:, hidden:], by_rows, preferred_element_type=F32
    )
    high, low = where_ref[0], where_ref[1]
    n_term, rank, _ = term_ref.shape
    part = rank // n_piece
    for k, out in enumerate(part_refs):
        column = jnp.bitwise_and(low + k, 3)
        for h in range(2):
            first = (jnp.bitwise_and(high + h, 1) * 4 + column) * part
            for n in range(n_term):
                out[h, n] = term_ref[n, pl.ds(pl.multiple_of(first, part), part), :].astype(
                    out.dtype
                )


def core(where, got, pre, pieces, hidden, rank):
    slots = pre.shape[0]
    n_piece = len(pieces)
    width = n_piece * LANES
    part = rank // n_piece
    return pl.pallas_call(
        functools.partial(core_kernel, n_piece, hidden),
        in_specs=[pl.BlockSpec(memory_space=pltpu.SMEM)]
        + [pl.BlockSpec(memory_space=pl.ANY)] * (2 + n_piece),
        out_shape=(
            jax.ShapeDtypeStruct((slots, 2 * hidden), BF16),
            *(
                jax.ShapeDtypeStruct((2, 3, part, hidden), F32 if k == 0 else BF16)
                for k in range(4)
            ),
        ),
        scratch_shapes=[
            pltpu.VMEM(got.shape, BF16),
            pltpu.VMEM(pre.shape, BF16),
            pltpu.VMEM((width, hidden + rank), BF16),
            pltpu.VMEM(got.shape, F32),
            pltpu.VMEM((slots, width), BF16),
            pltpu.VMEM((slots, width), BF16),
            pltpu.VMEM((3, rank, hidden), F32),
            pltpu.SemaphoreType.DMA((n_piece + 2,)),
        ],
        name="core",
    )(where, got, pre, *pieces)


def rows_kernel(n_piece, first, *refs):
    where_ref, both_ref = refs[:2]
    pieces = refs[2 : 2 + n_piece]
    row_ref, weights, wide, sems = refs[2 + n_piece :]
    slots = both_ref.shape[0]
    copies = fetch_pieces(where_ref, pieces, pl.ds(first, weights.shape[1]), weights, sems)
    for copy in copies:
        copy.wait()
    for c in range(0, n_piece, 2):
        rows = lax.dot_general(
            both_ref[...],
            weights[c * LANES : (c + 2) * LANES, :],
            (((1,), (1,)), ((), ())),
            preferred_element_type=F32,
        )
        wide[chunk_rows(c, slots, n_piece), :] = rows[:, :LANES]
        wide[chunk_rows(c + 1, slots, n_piece), :] = rows[:, LANES:]
    row_ref[...] = wide[...].astype(BF16)


def row_grads(where, both, pieces, first):
    slots, inner = both.shape
    n_piece = len(pieces)
    rows = slots * n_piece
    return pl.pallas_call(
        functools.partial(rows_kernel, n_piece, first),
        in_specs=[pl.BlockSpec(memory_space=pltpu.SMEM), pl.BlockSpec(memory_space=pltpu.VMEM)]
        + [pl.BlockSpec(memory_space=pl.ANY)] * n_piece,
        out_shape=jax.ShapeDtypeStruct((rows, LANES), BF16),
        scratch_shapes=[
            pltpu.VMEM((n_piece * LANES, inner), BF16),
            pltpu.VMEM((rows, LANES), F32),
            pltpu.SemaphoreType.DMA((n_piece,)),
        ],
        name="row_grads",
    )(where, both, *pieces)


def take_pair(wide_ref, first, second, slots, step):
    return jnp.concatenate(
        [
            wide_ref[chunk_rows(first, slots, step), :],
            wide_ref[chunk_rows(second, slots, step), :],
        ],
        axis=1,
    ).astype(BF16)


def combine_kernel(match_ref, got_ref, out_ref, wide_ref):
    slots = match_ref.shape[0]
    n_chunk = out_ref.shape[1] // LANES
    wide_ref[...] = got_ref[...].astype(F32)
    for c in range(0, n_chunk, 2):
        rows = take_pair(wide_ref, c, c + 1, slots, n_chunk)
        total = lax.dot_general(
            match_ref[...], rows, (((0,), (0,)), ((), ())), preferred_element_type=F32
        )
        out_ref[:, c * LANES : (c + 2) * LANES] = total.astype(BF16)


def combine(match, got, width):
    n_tok = match.shape[1]
    return pl.pallas_call(
        combine_kernel,
        out_shape=jax.ShapeDtypeStruct((n_tok, width), BF16),
        scratch_shapes=[pltpu.VMEM(got.shape, F32)],
        name="combine",
    )(match, got)


def swap(value):
    return lax.ppermute(value, "dp_0", [(0, 1), (1, 0)])


def shifted(value):
    size = lax.axis_size("dp_1")
    return [
        lax.ppermute(value, "dp_1", [(i, (i + k) % size) for i in range(size)])
        for k in range(1, size)
    ]


def exchange(value, n_owner):
    rows, lanes = value.shape
    out = lax.all_to_all(
        value.reshape(n_owner, rows // n_owner, lanes), "expert", 0, 0, tiled=True
    )
    return out.reshape(rows, lanes)


def body(
    tokens, out_grad, expert_ids, gate_probs, saved_pre, gate_weight, up_weight, down_weight, basis
):
    n_owner = lax.axis_size("expert")
    width = tokens.shape[1]
    slots = saved_pre.shape[2]
    cap = slots // n_owner
    hidden = gate_weight.shape[2]
    where = jnp.stack([lax.axis_index("dp_0"), lax.axis_index("dp_1")]).astype(jnp.int32)

    own = jnp.concatenate([down_weight[0], basis[0], gate_weight[0], up_weight[0]], axis=1)
    far = swap(own)
    sent, match = pack(expert_ids.T, gate_probs.T, tokens, out_grad, n_owner, cap)
    got = exchange(sent, n_owner)
    owns = [own] + shifted(own)
    fars = [far] + shifted(far)
    pieces = [piece for pair in zip(owns, fars) for piece in pair]
    rank = basis.shape[2]
    both, *parts = core(where, got, saved_pre[0, 0], pieces, hidden, rank)
    size = lax.axis_size("dp_1")
    summed = parts[0]
    for k in range(1, size):
        part = lax.ppermute(parts[k], "dp_1", [(i, (i + k) % size) for i in range(size)])
        summed = summed + part.astype(F32)
    row_grad = row_grads(where, both, pieces, hidden + rank)
    back = exchange(row_grad, n_owner)
    other = swap(summed[1].astype(BF16))
    proj_grads = (summed[0] + other.astype(F32))[None]
    in_grad = combine(match, back, width)
    return in_grad, proj_grads


def solution(mesh):
    finer = Mesh(mesh.devices.reshape(2, 4, mesh.shape["expert"]), DP_EXPERT)
    placed = (
        P(DP_EXPERT, None),
        P(DP_EXPERT, None),
        P(DP_EXPERT, None),
        P(DP_EXPERT, None),
        P(DP, "expert", None, None),
        P("expert", DP, None),
        P("expert", DP, None),
        P("expert", DP, None),
        P("expert", DP, None),
    )
    return jax.shard_map(
        body,
        mesh=finer,
        in_specs=placed,
        out_specs=(P(DP_EXPERT, None), P("expert", None, DP, None)),
        check_vma=False,
    )
```

```python
import functools

import jax
import jax.numpy as jnp
from jax import lax
from jax.experimental import pallas as pl
from jax.experimental.pallas import tpu as pltpu
from jax.sharding import Mesh
from jax.sharding import PartitionSpec as P


DP = ("dp_0", "dp_1")
DP_EXPERT = ("dp_0", "dp_1", "expert")
F32 = jnp.float32
BF16 = jnp.bfloat16
LANES = 128


def chunk_rows(start, slots, step):
    return pl.ds(start, slots, stride=step)


def pack_kernel(cap, ids_ref, probs_ref, tok_ref, grad_ref, out_ref, match_ref, wide_ref):
    slots, n_tok = match_ref.shape
    topk = ids_ref.shape[0]
    n_owner = slots // cap
    ids = ids_ref[...]
    probs = probs_ref[...]
    owner = lax.broadcasted_iota(jnp.int32, (n_owner, n_tok), 0)
    named = [owner == ids[k : k + 1, :] for k in range(topk)]
    per_owner = sum(n.astype(F32) for n in named)
    earlier = (
        lax.broadcasted_iota(jnp.int32, (n_tok, n_tok), 0)
        < lax.broadcasted_iota(jnp.int32, (n_tok, n_tok), 1)
    ).astype(F32)
    before = jnp.dot(per_owner.astype(BF16), earlier.astype(BF16), preferred_element_type=F32)
    slot = lax.broadcasted_iota(jnp.int32, (slots, n_tok), 0)
    match = jnp.zeros((slots, n_tok), F32)
    weight = jnp.zeros((slots, n_tok), F32)
    for k in range(topk):
        position = jnp.sum(jnp.where(named[k], before, 0.0), axis=0, keepdims=True)
        here = slot == ids[k : k + 1, :] * cap + position.astype(jnp.int32)
        match = match + here.astype(F32)
        weight = weight + jnp.where(here, probs[k : k + 1, :], 0.0)
    weight = jnp.sum(weight, axis=1, keepdims=True)
    match = match.astype(BF16)
    match_ref[...] = match
    n_chunk = tok_ref.shape[1] // LANES
    for half, src in enumerate((tok_ref, grad_ref)):
        for c in range(0, n_chunk, 2):
            rows = jnp.dot(
                match, src[:, c * LANES : (c + 2) * LANES], preferred_element_type=F32
            )
            if half:
                rows = rows * weight
            for i in range(2):
                wide_ref[chunk_rows(half * n_chunk + c + i, slots, 2 * n_chunk), :] = rows[
                    :, i * LANES : (i + 1) * LANES
                ]
    out_ref[...] = wide_ref[...].astype(BF16)


def pack(ids, probs, tokens, out_grad, n_owner, cap):
    n_tok, width = tokens.shape
    slots = n_owner * cap
    rows = slots * 2 * width // LANES
    return pl.pallas_call(
        functools.partial(pack_kernel, cap),
        out_shape=(
            jax.ShapeDtypeStruct((rows, LANES), BF16),
            jax.ShapeDtypeStruct((slots, n_tok), BF16),
        ),
        scratch_shapes=[pltpu.VMEM((rows, LANES), F32)],
        name="pack",
    )(ids, probs, tokens, out_grad)


def near(value):
    return pltpu.with_memory_space_constraint(value, pltpu.VMEM)


def in_vmem():
    return pl.BlockSpec(memory_space=pltpu.VMEM)


def in_place():
    return pl.BlockSpec(memory_space=pl.ANY)


def fetch(where_ref, pieces, places, columns, into, sems, at):
    high, low = where_ref[0], where_ref[1]
    copies = []
    for i, (piece, (other, k, first)) in enumerate(zip(pieces, places)):
        block = jnp.bitwise_and(high + other, 1) * 4 + jnp.bitwise_and(low + 4 - k, 3)
        rows = pl.ds(pl.multiple_of(block * LANES + first, LANES // 2), piece.shape[0])
        copy = pltpu.make_async_copy(piece.at[:, columns], into.at[rows, :], sems.at[at + i])
        copy.start()
        copies.append(copy)
    return copies


def fetch_all(sources, targets, sems, at):
    copies = []
    for i, (source, target) in enumerate(zip(sources, targets)):
        copy = pltpu.make_async_copy(source, target, sems.at[at + i])
        copy.start()
        copies.append(copy)
    return copies


def slopes_kernel(pre_ref, act_ref, slope_ref, hid_ref):
    hidden = act_ref.shape[1]
    gate = pre_ref[:, :hidden].astype(F32)
    up = pre_ref[:, hidden:].astype(F32)
    sig = jax.nn.sigmoid(gate)
    act = gate * sig
    act_ref[...] = act
    slope_ref[...] = up * sig * (1.0 + gate * (1.0 - sig))
    hid_ref[...] = (act * up).astype(BF16)


def slopes(pre):
    slots, both = pre.shape
    hidden = both // 2
    return pl.pallas_call(
        slopes_kernel,
        out_shape=(
            jax.ShapeDtypeStruct((slots, hidden), F32),
            jax.ShapeDtypeStruct((slots, hidden), F32),
            jax.ShapeDtypeStruct((slots, hidden), BF16),
        ),
        name="slopes",
    )(pre)


def spread(wide_ref, first, step, into):
    slots, width = into.shape
    for c in range(width // LANES):
        into[:, c * LANES : (c + 1) * LANES] = wide_ref[
            chunk_rows(first + c, slots, step), :
        ].astype(BF16)


def grads_kernel(places, *refs):
    n = len(places)
    where_ref, got_ref, act_hbm, slope_hbm = refs[:4]
    pieces = refs[4 : 4 + n]
    row_ref, both_ref, proj_ref = refs[4 + n : 7 + n]
    wide, dy_rows, rows_wide, w1, w2, act, slope, sems = refs[7 + n :]
    hidden = act.shape[1]
    slots, width = dy_rows.shape
    n_chunk = width // LANES
    first = fetch(where_ref, pieces, places, pl.ds(0, w1.shape[1]), w1, sems, 0)
    middle = fetch_all((slope_hbm, act_hbm), (slope, act), sems, 2 * n)
    last = fetch(where_ref, pieces, places, pl.ds(w1.shape[1], w2.shape[1]), w2, sems, n)
    wide[...] = got_ref[...].astype(F32)
    spread(wide, n_chunk, 2 * n_chunk, dy_rows)
    for copy in first:
        copy.wait()
    grad = jnp.dot(dy_rows[...], w1[:, :hidden], preferred_element_type=F32)
    for copy in middle:
        copy.wait()
    both_ref[:, :hidden] = (grad * slope[...]).astype(BF16)
    both_ref[:, hidden:] = (grad * act[...]).astype(BF16)
    for copy in last:
        copy.wait()
    for c in range(0, n_chunk, 2):
        rows = lax.dot_general(
            both_ref[...],
            w2[c * LANES : (c + 2) * LANES, :],
            (((1,), (1,)), ((), ())),
            preferred_element_type=F32,
        )
        rows_wide[chunk_rows(c, slots, n_chunk), :] = rows[:, :LANES]
        rows_wide[chunk_rows(c + 1, slots, n_chunk), :] = rows[:, LANES:]
    row_ref[...] = rows_wide[...].astype(BF16)
    proj_ref[...] = jnp.dot(dy_rows[...], w1[:, hidden:], preferred_element_type=F32).astype(BF16)


def grads(where, got, act, slope, pieces, places, rank):
    slots, hidden = act.shape
    width = got.shape[0] * LANES // slots // 2
    rows = slots * width // LANES
    n = len(pieces)
    return pl.pallas_call(
        functools.partial(grads_kernel, places),
        in_specs=[pl.BlockSpec(memory_space=pltpu.SMEM), in_vmem()] + [in_place()] * (2 + n),
        out_shape=(
            jax.ShapeDtypeStruct((rows, LANES), BF16),
            jax.ShapeDtypeStruct((slots, 2 * hidden), BF16),
            jax.ShapeDtypeStruct((slots, rank), BF16),
        ),
        scratch_shapes=[
            pltpu.VMEM(got.shape, F32),
            pltpu.VMEM((slots, width), BF16),
            pltpu.VMEM((rows, LANES), F32),
            pltpu.VMEM((width, hidden + rank), BF16),
            pltpu.VMEM((width, 2 * hidden), BF16),
            pltpu.VMEM((slots, hidden), F32),
            pltpu.VMEM((slots, hidden), F32),
            pltpu.SemaphoreType.DMA((2 * n + 2,)),
        ],
        name="grads",
    )(where, near(got), act, slope, *pieces)


def terms_kernel(places, first_column, *refs):
    n = len(places)
    where_ref, got_hbm, both_hbm, proj_hbm, hid_hbm = refs[:5]
    pieces = refs[5 : 5 + n]
    part_refs = refs[5 + n : 9 + n]
    got, both, proj, hid, basis, wide, x_rows, term_ref, sems = refs[9 + n :]
    hidden = hid.shape[1]
    n_chunk = x_rows.shape[1] // LANES
    (first,) = fetch_all((got_hbm,), (got,), sems, n)
    middle = fetch(
        where_ref, pieces, places, pl.ds(first_column, basis.shape[1]), basis, sems, 0
    )
    last = fetch_all((both_hbm, proj_hbm, hid_hbm), (both, proj, hid), sems, n + 1)
    first.wait()
    wide[...] = got[...].astype(F32)
    spread(wide, 0, 2 * n_chunk, x_rows)
    for copy in middle:
        copy.wait()
    x_proj = jnp.dot(x_rows[...], basis[...], preferred_element_type=F32).astype(BF16)
    for copy in last:
        copy.wait()
    by_rows = (((0,), (0,)), ((), ()))
    term_ref[0] = lax.dot_general(x_proj, both[:, :hidden], by_rows, preferred_element_type=F32)
    term_ref[1] = lax.dot_general(x_proj, both[:, hidden:], by_rows, preferred_element_type=F32)
    term_ref[2] = lax.dot_general(proj[...], hid[...], by_rows, preferred_element_type=F32)
    high, low = where_ref[0], where_ref[1]
    n_term, rank, _ = term_ref.shape
    part = rank // n_chunk
    for k, out in enumerate(part_refs):
        column = jnp.bitwise_and(low + k, 3)
        for h in range(2):
            begin = (jnp.bitwise_and(high + h, 1) * 4 + column) * part
            for t in range(n_term):
                out[h, t] = term_ref[t, pl.ds(pl.multiple_of(begin, part), part), :].astype(
                    out.dtype
                )


def terms(where, got, both, proj, hid, pieces, places):
    slots, hidden = hid.shape
    rank = proj.shape[1]
    width = got.shape[0] * LANES // slots // 2
    part = rank * LANES // width
    n = len(pieces)
    return pl.pallas_call(
        functools.partial(terms_kernel, places, hidden),
        in_specs=[pl.BlockSpec(memory_space=pltpu.SMEM)] + [in_place()] * (4 + n),
        out_shape=tuple(
            jax.ShapeDtypeStruct((2, 3, part, hidden), F32 if k == 0 else BF16) for k in range(4)
        ),
        scratch_shapes=[
            pltpu.VMEM(got.shape, BF16),
            pltpu.VMEM(both.shape, BF16),
            pltpu.VMEM(proj.shape, BF16),
            pltpu.VMEM(hid.shape, BF16),
            pltpu.VMEM((width, rank), BF16),
            pltpu.VMEM(got.shape, F32),
            pltpu.VMEM((slots, width), BF16),
            pltpu.VMEM((3, rank, hidden), F32),
            pltpu.SemaphoreType.DMA((n + 4,)),
        ],
        name="terms",
    )(where, got, both, proj, hid, *pieces)


def take_pair(wide_ref, first, second, slots, step):
    return jnp.concatenate(
        [
            wide_ref[chunk_rows(first, slots, step), :],
            wide_ref[chunk_rows(second, slots, step), :],
        ],
        axis=1,
    ).astype(BF16)


def combine_kernel(match_ref, got_ref, out_ref, wide_ref):
    slots = match_ref.shape[0]
    n_chunk = out_ref.shape[1] // LANES
    wide_ref[...] = got_ref[...].astype(F32)
    for c in range(0, n_chunk, 2):
        rows = take_pair(wide_ref, c, c + 1, slots, n_chunk)
        total = lax.dot_general(
            match_ref[...], rows, (((0,), (0,)), ((), ())), preferred_element_type=F32
        )
        out_ref[:, c * LANES : (c + 2) * LANES] = total.astype(BF16)


def combine(match, got, width):
    n_tok = match.shape[1]
    return pl.pallas_call(
        combine_kernel,
        out_shape=jax.ShapeDtypeStruct((n_tok, width), BF16),
        scratch_shapes=[pltpu.VMEM(got.shape, F32)],
        name="combine",
    )(match, near(got))


def swap(value):
    return lax.ppermute(value, "dp_0", [(0, 1), (1, 0)])


def shifted(value, k):
    size = lax.axis_size("dp_1")
    return lax.ppermute(value, "dp_1", [(i, (i + k) % size) for i in range(size)])


def exchange(value, n_owner):
    rows, lanes = value.shape
    out = lax.all_to_all(
        value.reshape(n_owner, rows // n_owner, lanes), "expert", 0, 0, tiled=True
    )
    return out.reshape(rows, lanes)


def body(
    tokens, out_grad, expert_ids, gate_probs, saved_pre, gate_weight, up_weight, down_weight, basis
):
    n_owner = lax.axis_size("expert")
    width = tokens.shape[1]
    slots = saved_pre.shape[2]
    cap = slots // n_owner
    where = jnp.stack([lax.axis_index("dp_0"), lax.axis_index("dp_1")]).astype(jnp.int32)

    own = jnp.concatenate([down_weight[0], basis[0], gate_weight[0], up_weight[0]], axis=1)
    far = swap(own)
    sent, match = pack(expert_ids.T, gate_probs.T, tokens, out_grad, n_owner, cap)
    got = exchange(sent, n_owner)
    pieces, places = [], []
    half = own.shape[0] // 2
    for other, block in enumerate((own, far)):
        left, right = shifted(block, 1), shifted(block, -1)
        top, bottom = shifted(left[:half], 1), shifted(right[half:], -1)
        pieces += [block, left, right, top, bottom]
        places += [(other, 0, 0), (other, 1, 0), (other, 3, 0), (other, 2, 0), (other, 2, half)]
    rank = basis.shape[2]
    act, slope, hid = slopes(saved_pre[0, 0])
    places = tuple(places)
    row_grad, both, proj = grads(where, got, act, slope, pieces, places, rank)
    back = exchange(row_grad, n_owner)
    parts = terms(where, got, both, proj, hid, pieces, places)
    size = lax.axis_size("dp_1")
    summed = parts[0]
    for k in range(1, size):
        summed = summed + shifted(parts[k], k).astype(F32)
    other = swap(summed[1].astype(BF16))
    proj_grads = (summed[0] + other.astype(F32))[None]
    in_grad = combine(match, back, width)
    return in_grad, proj_grads


def solution(mesh):
    finer = Mesh(mesh.devices.reshape(2, 4, mesh.shape["expert"]), DP_EXPERT)
    placed = (
        P(DP_EXPERT, None),
        P(DP_EXPERT, None),
        P(DP_EXPERT, None),
        P(DP_EXPERT, None),
        P(DP, "expert", None, None),
        P("expert", DP, None),
        P("expert", DP, None),
        P("expert", DP, None),
        P("expert", DP, None),
    )
    return jax.shard_map(
        body,
        mesh=finer,
        in_specs=placed,
        out_specs=(P(DP_EXPERT, None), P("expert", None, DP, None)),
        check_vma=False,
    )
```

```python
import functools

import jax
import jax.numpy as jnp
from jax import lax
from jax.experimental import pallas as pl
from jax.experimental.pallas import tpu as pltpu
from jax.sharding import Mesh
from jax.sharding import PartitionSpec as P


DP = ("dp_0", "dp_1")
DP_EXPERT = ("dp_0", "dp_1", "expert")
F32 = jnp.float32
BF16 = jnp.bfloat16
LANES = 128


def chunk_rows(start, slots, step):
    return pl.ds(start, slots, stride=step)


def pack_kernel(cap, ids_ref, probs_ref, tok_ref, grad_ref, out_ref, match_ref, wide_ref):
    slots, n_tok = match_ref.shape
    topk = ids_ref.shape[0]
    n_owner = slots // cap
    ids = ids_ref[...]
    probs = probs_ref[...]
    owner = lax.broadcasted_iota(jnp.int32, (n_owner, n_tok), 0)
    named = [owner == ids[k : k + 1, :] for k in range(topk)]
    per_owner = sum(n.astype(F32) for n in named)
    earlier = (
        lax.broadcasted_iota(jnp.int32, (n_tok, n_tok), 0)
        < lax.broadcasted_iota(jnp.int32, (n_tok, n_tok), 1)
    ).astype(F32)
    before = jnp.dot(per_owner.astype(BF16), earlier.astype(BF16), preferred_element_type=F32)
    slot = lax.broadcasted_iota(jnp.int32, (slots, n_tok), 0)
    match = jnp.zeros((slots, n_tok), F32)
    weight = jnp.zeros((slots, n_tok), F32)
    for k in range(topk):
        position = jnp.sum(jnp.where(named[k], before, 0.0), axis=0, keepdims=True)
        here = slot == ids[k : k + 1, :] * cap + position.astype(jnp.int32)
        match = match + here.astype(F32)
        weight = weight + jnp.where(here, probs[k : k + 1, :], 0.0)
    weight = jnp.sum(weight, axis=1, keepdims=True)
    match = match.astype(BF16)
    match_ref[...] = match
    n_chunk = tok_ref.shape[1] // LANES
    for half, src in enumerate((tok_ref, grad_ref)):
        for c in range(0, n_chunk, 2):
            rows = jnp.dot(
                match, src[:, c * LANES : (c + 2) * LANES], preferred_element_type=F32
            )
            if half:
                rows = rows * weight
            for i in range(2):
                wide_ref[chunk_rows(half * n_chunk + c + i, slots, 2 * n_chunk), :] = rows[
                    :, i * LANES : (i + 1) * LANES
                ]
    out_ref[...] = wide_ref[...].astype(BF16)


def pack(ids, probs, tokens, out_grad, n_owner, cap):
    n_tok, width = tokens.shape
    slots = n_owner * cap
    rows = slots * 2 * width // LANES
    return pl.pallas_call(
        functools.partial(pack_kernel, cap),
        out_shape=(
            jax.ShapeDtypeStruct((rows, LANES), BF16),
            jax.ShapeDtypeStruct((slots, n_tok), BF16),
        ),
        scratch_shapes=[pltpu.VMEM((rows, LANES), F32)],
        name="pack",
    )(ids, probs, tokens, out_grad)


def near(value):
    return pltpu.with_memory_space_constraint(value, pltpu.VMEM)


def in_vmem():
    return pl.BlockSpec(memory_space=pltpu.VMEM)


def in_place():
    return pl.BlockSpec(memory_space=pl.ANY)


def fetch(where_ref, pieces, places, columns, into, sems, at):
    high, low = where_ref[0], where_ref[1]
    copies = []
    for i, (piece, (other, k, first)) in enumerate(zip(pieces, places)):
        block = jnp.bitwise_and(high + other, 1) * 4 + jnp.bitwise_and(low + 4 - k, 3)
        rows = pl.ds(pl.multiple_of(block * LANES + first, LANES // 2), piece.shape[0])
        copy = pltpu.make_async_copy(piece.at[:, columns], into.at[rows, :], sems.at[at + i])
        copy.start()
        copies.append(copy)
    return copies


def fetch_all(sources, targets, sems, at):
    copies = []
    for i, (source, target) in enumerate(zip(sources, targets)):
        copy = pltpu.make_async_copy(source, target, sems.at[at + i])
        copy.start()
        copies.append(copy)
    return copies


def slopes_kernel(pre_ref, act_ref, slope_ref, hid_ref):
    hidden = act_ref.shape[1]
    gate = pre_ref[:, :hidden].astype(F32)
    up = pre_ref[:, hidden:].astype(F32)
    sig = jax.nn.sigmoid(gate)
    act = gate * sig
    act_ref[...] = act
    slope_ref[...] = up * sig * (1.0 + gate * (1.0 - sig))
    hid_ref[...] = (act * up).astype(BF16)


def slopes(pre):
    slots, both = pre.shape
    hidden = both // 2
    return pl.pallas_call(
        slopes_kernel,
        out_shape=(
            jax.ShapeDtypeStruct((slots, hidden), F32),
            jax.ShapeDtypeStruct((slots, hidden), F32),
            jax.ShapeDtypeStruct((slots, hidden), BF16),
        ),
        name="slopes",
    )(pre)


def spread(wide_ref, first, step, into):
    slots, width = into.shape
    for c in range(width // LANES):
        into[:, c * LANES : (c + 1) * LANES] = wide_ref[
            chunk_rows(first + c, slots, step), :
        ].astype(BF16)


def grads_kernel(places, *refs):
    n = len(places)
    where_ref, got_ref, act_hbm, slope_hbm = refs[:4]
    pieces = refs[4 : 4 + n]
    row_hbm, both_hbm, proj_hbm = refs[4 + n : 7 + n]
    wide, x_rows, dy_rows, rows_wide, w1, w2, act, slope, row, both, proj, sems = refs[7 + n :]
    hidden = act.shape[1]
    slots, width = dy_rows.shape
    n_chunk = width // LANES
    first = fetch(where_ref, pieces, places, pl.ds(0, w1.shape[1]), w1, sems, 0)
    middle = fetch_all((slope_hbm, act_hbm), (slope, act), sems, 2 * n)
    last = fetch(where_ref, pieces, places, pl.ds(w1.shape[1], w2.shape[1]), w2, sems, n)
    wide[...] = got_ref[...].astype(F32)
    spread(wide, n_chunk, 2 * n_chunk, dy_rows)
    spread(wide, 0, 2 * n_chunk, x_rows)
    for copy in first:
        copy.wait()
    grad = jnp.dot(dy_rows[...], w1[:, :hidden], preferred_element_type=F32)
    for copy in middle:
        copy.wait()
    both[:, :hidden] = (grad * slope[...]).astype(BF16)
    both[:, hidden:] = (grad * act[...]).astype(BF16)
    proj[0] = jnp.dot(x_rows[...], w1[:, hidden:], preferred_element_type=F32).astype(BF16)
    proj[1] = jnp.dot(dy_rows[...], w1[:, hidden:], preferred_element_type=F32).astype(BF16)
    sent = fetch_all((both, proj), (both_hbm, proj_hbm), sems, 2 * n + 2)
    for copy in last:
        copy.wait()
    for c in range(0, n_chunk, 2):
        rows = lax.dot_general(
            both[...],
            w2[c * LANES : (c + 2) * LANES, :],
            (((1,), (1,)), ((), ())),
            preferred_element_type=F32,
        )
        rows_wide[chunk_rows(c, slots, n_chunk), :] = rows[:, :LANES]
        rows_wide[chunk_rows(c + 1, slots, n_chunk), :] = rows[:, LANES:]
    size = row.shape[0] // 2
    for i in range(2):
        here = slice(i * size, (i + 1) * size)
        row[here, :] = rows_wide[here, :].astype(BF16)
        sent += fetch_all((row.at[here, :],), (row_hbm.at[here, :],), sems, 2 * n + 4 + i)
    for copy in sent:
        copy.wait()


def grads(where, got, act, slope, pieces, places, rank):
    slots, hidden = act.shape
    width = got.shape[0] * LANES // slots // 2
    rows = slots * width // LANES
    n = len(pieces)
    return pl.pallas_call(
        functools.partial(grads_kernel, places),
        in_specs=[pl.BlockSpec(memory_space=pltpu.SMEM), in_vmem()] + [in_place()] * (2 + n),
        out_specs=(in_place(),) * 3,
        out_shape=(
            jax.ShapeDtypeStruct((rows, LANES), BF16),
            jax.ShapeDtypeStruct((slots, 2 * hidden), BF16),
            jax.ShapeDtypeStruct((2, slots, rank), BF16),
        ),
        scratch_shapes=[
            pltpu.VMEM(got.shape, F32),
            pltpu.VMEM((slots, width), BF16),
            pltpu.VMEM((slots, width), BF16),
            pltpu.VMEM((rows, LANES), F32),
            pltpu.VMEM((width, hidden + rank), BF16),
            pltpu.VMEM((width, 2 * hidden), BF16),
            pltpu.VMEM((slots, hidden), F32),
            pltpu.VMEM((slots, hidden), F32),
            pltpu.VMEM((rows, LANES), BF16),
            pltpu.VMEM((slots, 2 * hidden), BF16),
            pltpu.VMEM((2, slots, rank), BF16),
            pltpu.SemaphoreType.DMA((2 * n + 6,)),
        ],
        name="grads",
    )(where, near(got), act, slope, *pieces)


def terms_kernel(where_ref, both_hbm, proj_hbm, hid_hbm, *refs):
    part_refs = refs[:4]
    both, proj, hid, term_ref, sems = refs[4:]
    hidden = hid.shape[1]
    proj_in, both_in, hid_in = fetch_all(
        (proj_hbm, both_hbm, hid_hbm), (proj, both, hid), sems, 0
    )
    by_rows = (((0,), (0,)), ((), ()))
    proj_in.wait()
    both_in.wait()
    x_proj = proj[0]
    term_ref[0] = lax.dot_general(x_proj, both[:, :hidden], by_rows, preferred_element_type=F32)
    term_ref[1] = lax.dot_general(x_proj, both[:, hidden:], by_rows, preferred_element_type=F32)
    hid_in.wait()
    term_ref[2] = lax.dot_general(proj[1], hid[...], by_rows, preferred_element_type=F32)
    high, low = where_ref[0], where_ref[1]
    n_term, part = term_ref.shape[0], part_refs[0].shape[2]
    for k, out in enumerate(part_refs):
        column = jnp.bitwise_and(low + k, 3)
        for h in range(2):
            begin = (jnp.bitwise_and(high + h, 1) * 4 + column) * part
            for t in range(n_term):
                out[h, t] = term_ref[t, pl.ds(pl.multiple_of(begin, part), part), :].astype(
                    out.dtype
                )


def terms(where, both, proj, hid, n_dp):
    _, hidden = hid.shape
    rank = proj.shape[2]
    part = rank // n_dp
    return pl.pallas_call(
        terms_kernel,
        in_specs=[pl.BlockSpec(memory_space=pltpu.SMEM)] + [in_place()] * 3,
        out_shape=tuple(
            jax.ShapeDtypeStruct((2, 3, part, hidden), F32 if k == 0 else BF16) for k in range(4)
        ),
        scratch_shapes=[
            pltpu.VMEM(both.shape, BF16),
            pltpu.VMEM(proj.shape, BF16),
            pltpu.VMEM(hid.shape, BF16),
            pltpu.VMEM((3, rank, hidden), F32),
            pltpu.SemaphoreType.DMA((3,)),
        ],
        name="terms",
    )(where, both, proj, hid)


def take_pair(wide_ref, first, second, slots, step):
    return jnp.concatenate(
        [
            wide_ref[chunk_rows(first, slots, step), :],
            wide_ref[chunk_rows(second, slots, step), :],
        ],
        axis=1,
    ).astype(BF16)


def combine_kernel(match_ref, got_ref, out_ref, wide_ref):
    slots = match_ref.shape[0]
    n_chunk = out_ref.shape[1] // LANES
    wide_ref[...] = got_ref[...].astype(F32)
    for c in range(0, n_chunk, 2):
        rows = take_pair(wide_ref, c, c + 1, slots, n_chunk)
        total = lax.dot_general(
            match_ref[...], rows, (((0,), (0,)), ((), ())), preferred_element_type=F32
        )
        out_ref[:, c * LANES : (c + 2) * LANES] = total.astype(BF16)


def combine(match, got, width):
    n_tok = match.shape[1]
    return pl.pallas_call(
        combine_kernel,
        out_shape=jax.ShapeDtypeStruct((n_tok, width), BF16),
        scratch_shapes=[pltpu.VMEM(got.shape, F32)],
        name="combine",
    )(match, near(got))


def swap(value):
    return lax.ppermute(value, "dp_0", [(0, 1), (1, 0)])


def shifted(value, k):
    size = lax.axis_size("dp_1")
    return lax.ppermute(value, "dp_1", [(i, (i + k) % size) for i in range(size)])


def exchange(value, n_owner):
    rows, lanes = value.shape
    out = lax.all_to_all(
        value.reshape(n_owner, rows // n_owner, lanes), "expert", 0, 0, tiled=True
    )
    return out.reshape(rows, lanes)


def body(
    tokens, out_grad, expert_ids, gate_probs, saved_pre, gate_weight, up_weight, down_weight, basis
):
    n_owner = lax.axis_size("expert")
    width = tokens.shape[1]
    slots = saved_pre.shape[2]
    cap = slots // n_owner
    where = jnp.stack([lax.axis_index("dp_0"), lax.axis_index("dp_1")]).astype(jnp.int32)

    own = jnp.concatenate([down_weight[0], basis[0], gate_weight[0], up_weight[0]], axis=1)
    far = swap(own)
    sent, match = pack(expert_ids.T, gate_probs.T, tokens, out_grad, n_owner, cap)
    got = exchange(sent, n_owner)
    pieces, places = [], []
    half = own.shape[0] // 2
    for other, block in enumerate((own, far)):
        left, right = shifted(block, 1), shifted(block, -1)
        top, bottom = shifted(left[:half], 1), shifted(right[half:], -1)
        pieces += [block, left, right, top, bottom]
        places += [(other, 0, 0), (other, 1, 0), (other, 3, 0), (other, 2, 0), (other, 2, half)]
    rank = basis.shape[2]
    act, slope, hid = slopes(saved_pre[0, 0])
    places = tuple(places)
    row_grad, both, proj = grads(where, got, act, slope, pieces, places, rank)
    back = exchange(row_grad, n_owner)
    parts = terms(where, both, proj, hid, 8)
    summed = parts[0]
    for k in (2, 1, 3):
        summed = summed + shifted(parts[k], k).astype(F32)
    other = swap(summed[1].astype(BF16))
    proj_grads = (summed[0] + other.astype(F32))[None]
    in_grad = combine(match, back, width)
    return in_grad, proj_grads


def solution(mesh):
    finer = Mesh(mesh.devices.reshape(2, 4, mesh.shape["expert"]), DP_EXPERT)
    placed = (
        P(DP_EXPERT, None),
        P(DP_EXPERT, None),
        P(DP_EXPERT, None),
        P(DP_EXPERT, None),
        P(DP, "expert", None, None),
        P("expert", DP, None),
        P("expert", DP, None),
        P("expert", DP, None),
        P("expert", DP, None),
    )
    return jax.shard_map(
        body,
        mesh=finer,
        in_specs=placed,
        out_specs=(P(DP_EXPERT, None), P("expert", None, DP, None)),
        check_vma=False,
    )
```

```python
import functools

import jax
import jax.numpy as jnp
from jax import lax
from jax.experimental import pallas as pl
from jax.experimental.pallas import tpu as pltpu
from jax.sharding import Mesh
from jax.sharding import PartitionSpec as P


DP = ("dp_0", "dp_1")
DP_EXPERT = ("dp_0", "dp_1", "expert")
F32 = jnp.float32
BF16 = jnp.bfloat16
LANES = 128


def chunk_rows(start, slots, step):
    return pl.ds(start, slots, stride=step)


def write_rows(rows, first, wide_ref, step):
    slots = rows.shape[0]
    for i in range(rows.shape[1] // LANES):
        wide_ref[chunk_rows(first + i, slots, step), :] = rows[:, i * LANES : (i + 1) * LANES]


def pack_grad_kernel(cap, ids_ref, probs_ref, grad_ref, out_ref, match_ref, wide_ref):
    slots, n_tok = match_ref.shape
    topk = ids_ref.shape[0]
    n_owner = slots // cap
    ids = ids_ref[...]
    probs = probs_ref[...]
    owner = lax.broadcasted_iota(jnp.int32, (n_owner, n_tok), 0)
    named = [owner == ids[k : k + 1, :] for k in range(topk)]
    per_owner = sum(n.astype(F32) for n in named)
    earlier = (
        lax.broadcasted_iota(jnp.int32, (n_tok, n_tok), 0)
        < lax.broadcasted_iota(jnp.int32, (n_tok, n_tok), 1)
    ).astype(F32)
    before = jnp.dot(per_owner.astype(BF16), earlier.astype(BF16), preferred_element_type=F32)
    slot = lax.broadcasted_iota(jnp.int32, (slots, n_tok), 0)
    match = jnp.zeros((slots, n_tok), F32)
    weight = jnp.zeros((slots, n_tok), F32)
    for k in range(topk):
        position = jnp.sum(jnp.where(named[k], before, 0.0), axis=0, keepdims=True)
        here = slot == ids[k : k + 1, :] * cap + position.astype(jnp.int32)
        match = match + here.astype(F32)
        weight = weight + jnp.where(here, probs[k : k + 1, :], 0.0)
    weight = jnp.sum(weight, axis=1, keepdims=True)
    match = match.astype(BF16)
    match_ref[...] = match
    n_chunk = grad_ref.shape[1] // LANES
    for c in range(0, n_chunk, 2):
        rows = jnp.dot(
            match, grad_ref[:, c * LANES : (c + 2) * LANES], preferred_element_type=F32
        )
        write_rows(rows * weight, c, wide_ref, n_chunk)
    out_ref[...] = wide_ref[...].astype(BF16)


def pack_grad(ids, probs, out_grad, n_owner, cap):
    n_tok, width = out_grad.shape
    slots = n_owner * cap
    rows = slots * width // LANES
    return pl.pallas_call(
        functools.partial(pack_grad_kernel, cap),
        out_shape=(
            jax.ShapeDtypeStruct((rows, LANES), BF16),
            jax.ShapeDtypeStruct((slots, n_tok), BF16),
        ),
        scratch_shapes=[pltpu.VMEM((rows, LANES), F32)],
        name="pack_grad",
    )(ids, probs, out_grad)


def pack_token_kernel(match_ref, tok_ref, out_ref, wide_ref):
    n_chunk = tok_ref.shape[1] // LANES
    for c in range(0, n_chunk, 2):
        rows = jnp.dot(
            match_ref[...], tok_ref[:, c * LANES : (c + 2) * LANES], preferred_element_type=F32
        )
        write_rows(rows, c, wide_ref, n_chunk)
    out_ref[...] = wide_ref[...].astype(BF16)


def pack_token(match, tokens):
    rows = match.shape[0] * tokens.shape[1] // LANES
    return pl.pallas_call(
        pack_token_kernel,
        out_shape=jax.ShapeDtypeStruct((rows, LANES), BF16),
        scratch_shapes=[pltpu.VMEM((rows, LANES), F32)],
        name="pack_token",
    )(match, tokens)


def near(value):
    return pltpu.with_memory_space_constraint(value, pltpu.VMEM)


def in_vmem():
    return pl.BlockSpec(memory_space=pltpu.VMEM)


def in_place():
    return pl.BlockSpec(memory_space=pl.ANY)


def fetch(where_ref, pieces, places, columns, into, sems, at):
    high, low = where_ref[0], where_ref[1]
    copies = []
    for i, (piece, (other, k, first)) in enumerate(zip(pieces, places)):
        block = jnp.bitwise_and(high + other, 1) * 4 + jnp.bitwise_and(low + 4 - k, 3)
        rows = pl.ds(pl.multiple_of(block * LANES + first, LANES // 2), piece.shape[0])
        copy = pltpu.make_async_copy(piece.at[:, columns], into.at[rows, :], sems.at[at + i])
        copy.start()
        copies.append(copy)
    return copies


def fetch_all(sources, targets, sems, at):
    copies = []
    for i, (source, target) in enumerate(zip(sources, targets)):
        copy = pltpu.make_async_copy(source, target, sems.at[at + i])
        copy.start()
        copies.append(copy)
    return copies


def slopes_kernel(pre_ref, act_ref, slope_ref, hid_ref):
    hidden = act_ref.shape[1]
    gate = pre_ref[:, :hidden].astype(F32)
    up = pre_ref[:, hidden:].astype(F32)
    sig = jax.nn.sigmoid(gate)
    act = gate * sig
    act_ref[...] = act
    slope_ref[...] = up * sig * (1.0 + gate * (1.0 - sig))
    hid_ref[...] = (act * up).astype(BF16)


def slopes(pre):
    slots, both = pre.shape
    hidden = both // 2
    return pl.pallas_call(
        slopes_kernel,
        out_shape=(
            jax.ShapeDtypeStruct((slots, hidden), F32),
            jax.ShapeDtypeStruct((slots, hidden), F32),
            jax.ShapeDtypeStruct((slots, hidden), BF16),
        ),
        name="slopes",
    )(pre)


def spread(wide_ref, into):
    slots, width = into.shape
    n_chunk = width // LANES
    for c in range(n_chunk):
        into[:, c * LANES : (c + 1) * LANES] = wide_ref[chunk_rows(c, slots, n_chunk), :].astype(
            BF16
        )


def grads_kernel(places, *refs):
    n = len(places)
    where_ref, got_ref, act_hbm, slope_hbm = refs[:4]
    pieces = refs[4 : 4 + n]
    row_hbm, both_hbm, proj_hbm = refs[4 + n : 7 + n]
    wide, dy_rows, rows_wide, w1, w2, act, slope, row, both, proj, sems = refs[7 + n :]
    hidden = act.shape[1]
    _, width = dy_rows.shape
    n_chunk = width // LANES
    first = fetch(where_ref, pieces, places, pl.ds(0, w1.shape[1]), w1, sems, 0)
    middle = fetch_all((slope_hbm, act_hbm), (slope, act), sems, 2 * n)
    last = fetch(where_ref, pieces, places, pl.ds(w1.shape[1], w2.shape[1]), w2, sems, n)
    wide[...] = got_ref[...].astype(F32)
    spread(wide, dy_rows)
    for copy in first:
        copy.wait()
    grad = jnp.dot(dy_rows[...], w1[:, :hidden], preferred_element_type=F32)
    for copy in middle:
        copy.wait()
    both[:, :hidden] = (grad * slope[...]).astype(BF16)
    both[:, hidden:] = (grad * act[...]).astype(BF16)
    for copy in last:
        copy.wait()
    for c in range(0, n_chunk, 2):
        rows = lax.dot_general(
            both[...],
            w2[c * LANES : (c + 2) * LANES, :],
            (((1,), (1,)), ((), ())),
            preferred_element_type=F32,
        )
        write_rows(rows, c, rows_wide, n_chunk)
    row[...] = rows_wide[...].astype(BF16)
    proj[...] = jnp.dot(dy_rows[...], w1[:, hidden:], preferred_element_type=F32).astype(BF16)
    for copy in fetch_all((row, both, proj), (row_hbm, both_hbm, proj_hbm), sems, 2 * n + 2):
        copy.wait()


def grads(where, got, act, slope, pieces, places, rank):
    slots, hidden = act.shape
    width = got.shape[0] * LANES // slots
    n = len(pieces)
    return pl.pallas_call(
        functools.partial(grads_kernel, places),
        in_specs=[pl.BlockSpec(memory_space=pltpu.SMEM), in_vmem()] + [in_place()] * (2 + n),
        out_specs=(in_place(),) * 3,
        out_shape=(
            jax.ShapeDtypeStruct(got.shape, BF16),
            jax.ShapeDtypeStruct((slots, 2 * hidden), BF16),
            jax.ShapeDtypeStruct((slots, rank), BF16),
        ),
        scratch_shapes=[
            pltpu.VMEM(got.shape, F32),
            pltpu.VMEM((slots, width), BF16),
            pltpu.VMEM(got.shape, F32),
            pltpu.VMEM((width, hidden + rank), BF16),
            pltpu.VMEM((width, 2 * hidden), BF16),
            pltpu.VMEM((slots, hidden), F32),
            pltpu.VMEM((slots, hidden), F32),
            pltpu.VMEM(got.shape, BF16),
            pltpu.VMEM((slots, 2 * hidden), BF16),
            pltpu.VMEM((slots, rank), BF16),
            pltpu.SemaphoreType.DMA((2 * n + 5,)),
        ],
        name="grads",
    )(where, near(got), act, slope, *pieces)


def terms_kernel(places, *refs):
    n = len(places)
    where_ref, got_ref, both_hbm, proj_hbm, hid_hbm = refs[:5]
    pieces = refs[5 : 5 + n]
    part_refs = refs[5 + n : 9 + n]
    both, proj, hid, basis, wide, x_rows, term_ref, sems = refs[9 + n :]
    hidden = hid.shape[1]
    columns = pl.ds(hidden, basis.shape[1])
    first = fetch(where_ref, pieces, places, columns, basis, sems, 0)
    proj_in, hid_in, both_in = fetch_all(
        (proj_hbm, hid_hbm, both_hbm), (proj, hid, both), sems, n
    )
    wide[...] = got_ref[...].astype(F32)
    spread(wide, x_rows)
    for copy in first:
        copy.wait()
    x_proj = jnp.dot(x_rows[...], basis[...], preferred_element_type=F32).astype(BF16)
    by_rows = (((0,), (0,)), ((), ()))
    proj_in.wait()
    hid_in.wait()
    term_ref[2] = lax.dot_general(proj[...], hid[...], by_rows, preferred_element_type=F32)
    both_in.wait()
    term_ref[0] = lax.dot_general(x_proj, both[:, :hidden], by_rows, preferred_element_type=F32)
    term_ref[1] = lax.dot_general(x_proj, both[:, hidden:], by_rows, preferred_element_type=F32)
    high, low = where_ref[0], where_ref[1]
    n_term, part = term_ref.shape[0], part_refs[0].shape[2]
    for k, out in enumerate(part_refs):
        column = jnp.bitwise_and(low + k, 3)
        for h in range(2):
            begin = (jnp.bitwise_and(high + h, 1) * 4 + column) * part
            for t in range(n_term):
                out[h, t] = term_ref[t, pl.ds(pl.multiple_of(begin, part), part), :].astype(
                    out.dtype
                )


def terms(where, got, both, proj, hid, pieces, places, n_dp):
    slots, hidden = hid.shape
    rank = proj.shape[1]
    width = got.shape[0] * LANES // slots
    part = rank // n_dp
    n = len(pieces)
    return pl.pallas_call(
        functools.partial(terms_kernel, places),
        in_specs=[pl.BlockSpec(memory_space=pltpu.SMEM), in_vmem()] + [in_place()] * (3 + n),
        out_shape=tuple(
            jax.ShapeDtypeStruct((2, 3, part, hidden), F32 if k == 0 else BF16) for k in range(4)
        ),
        scratch_shapes=[
            pltpu.VMEM(both.shape, BF16),
            pltpu.VMEM(proj.shape, BF16),
            pltpu.VMEM(hid.shape, BF16),
            pltpu.VMEM((width, rank), BF16),
            pltpu.VMEM(got.shape, F32),
            pltpu.VMEM((slots, width), BF16),
            pltpu.VMEM((3, rank, hidden), F32),
            pltpu.SemaphoreType.DMA((n + 3,)),
        ],
        name="terms",
    )(where, near(got), both, proj, hid, *pieces)


def take_pair(wide_ref, first, second, slots, step):
    return jnp.concatenate(
        [
            wide_ref[chunk_rows(first, slots, step), :],
            wide_ref[chunk_rows(second, slots, step), :],
        ],
        axis=1,
    ).astype(BF16)


def combine_kernel(match_ref, got_ref, out_ref, wide_ref):
    slots = match_ref.shape[0]
    n_chunk = out_ref.shape[1] // LANES
    wide_ref[...] = got_ref[...].astype(F32)
    for c in range(0, n_chunk, 2):
        rows = take_pair(wide_ref, c, c + 1, slots, n_chunk)
        total = lax.dot_general(
            match_ref[...], rows, (((0,), (0,)), ((), ())), preferred_element_type=F32
        )
        out_ref[:, c * LANES : (c + 2) * LANES] = total.astype(BF16)


def combine(match, got, width):
    n_tok = match.shape[1]
    return pl.pallas_call(
        combine_kernel,
        out_shape=jax.ShapeDtypeStruct((n_tok, width), BF16),
        scratch_shapes=[pltpu.VMEM(got.shape, F32)],
        name="combine",
    )(match, near(got))


def swap(value):
    return lax.ppermute(value, "dp_0", [(0, 1), (1, 0)])


def shifted(value, k):
    size = lax.axis_size("dp_1")
    return lax.ppermute(value, "dp_1", [(i, (i + k) % size) for i in range(size)])


def exchange(value, n_owner):
    rows, lanes = value.shape
    out = lax.all_to_all(
        value.reshape(n_owner, rows // n_owner, lanes), "expert", 0, 0, tiled=True
    )
    return out.reshape(rows, lanes)


def body(
    tokens, out_grad, expert_ids, gate_probs, saved_pre, gate_weight, up_weight, down_weight, basis
):
    n_owner = lax.axis_size("expert")
    width = tokens.shape[1]
    slots = saved_pre.shape[2]
    cap = slots // n_owner
    where = jnp.stack([lax.axis_index("dp_0"), lax.axis_index("dp_1")]).astype(jnp.int32)

    own = jnp.concatenate([down_weight[0], basis[0], gate_weight[0], up_weight[0]], axis=1)
    far = swap(own)
    sent_grad, match = pack_grad(expert_ids.T, gate_probs.T, out_grad, n_owner, cap)
    got_grad = exchange(sent_grad, n_owner)
    sent_token = pack_token(match, tokens)
    got_token = exchange(sent_token, n_owner)
    half = own.shape[0] // 2
    pieces = [own] + [shifted(own, k) for k in (2, 1, 3)]
    places = [(0, 0, 0), (0, 2, 0), (0, 1, 0), (0, 3, 0)]
    left, right = shifted(far, 1), shifted(far, -1)
    top, bottom = shifted(left[:half], 1), shifted(right[half:], -1)
    pieces += [far, left, right, top, bottom]
    places += [(1, 0, 0), (1, 1, 0), (1, 3, 0), (1, 2, 0), (1, 2, half)]
    places = tuple(places)
    rank = basis.shape[2]
    act, slope, hid = slopes(saved_pre[0, 0])
    row_grad, both, proj = grads(where, got_grad, act, slope, pieces, places, rank)
    back = exchange(row_grad, n_owner)
    parts = terms(where, got_token, both, proj, hid, pieces, places, 8)
    summed = parts[0]
    for k in (2, 1, 3):
        summed = summed + shifted(parts[k], k).astype(F32)
    other = swap(summed[1].astype(BF16))
    proj_grads = (summed[0] + other.astype(F32))[None]
    in_grad = combine(match, back, width)
    return in_grad, proj_grads


def solution(mesh):
    finer = Mesh(mesh.devices.reshape(2, 4, mesh.shape["expert"]), DP_EXPERT)
    placed = (
        P(DP_EXPERT, None),
        P(DP_EXPERT, None),
        P(DP_EXPERT, None),
        P(DP_EXPERT, None),
        P(DP, "expert", None, None),
        P("expert", DP, None),
        P("expert", DP, None),
        P("expert", DP, None),
        P("expert", DP, None),
    )
    return jax.shard_map(
        body,
        mesh=finer,
        in_specs=placed,
        out_specs=(P(DP_EXPERT, None), P("expert", None, DP, None)),
        check_vma=False,
    )
```

```python
import functools

import jax
import jax.numpy as jnp
from jax import lax
from jax.experimental import pallas as pl
from jax.experimental.pallas import tpu as pltpu
from jax.sharding import Mesh
from jax.sharding import PartitionSpec as P


DP = ("dp_0", "dp_1")
DP_EXPERT = ("dp_0", "dp_1", "expert")
F32 = jnp.float32
BF16 = jnp.bfloat16
LANES = 128


def chunk_rows(start, slots, step):
    return pl.ds(start, slots, stride=step)


def pack_kernel(cap, ids_ref, probs_ref, tok_ref, grad_ref, out_ref, match_ref, wide_ref):
    slots, n_tok = match_ref.shape
    topk = ids_ref.shape[0]
    n_owner = slots // cap
    ids = ids_ref[...]
    probs = probs_ref[...]
    owner = lax.broadcasted_iota(jnp.int32, (n_owner, n_tok), 0)
    named = [owner == ids[k : k + 1, :] for k in range(topk)]
    per_owner = sum(n.astype(F32) for n in named)
    earlier = (
        lax.broadcasted_iota(jnp.int32, (n_tok, n_tok), 0)
        < lax.broadcasted_iota(jnp.int32, (n_tok, n_tok), 1)
    ).astype(F32)
    before = jnp.dot(per_owner.astype(BF16), earlier.astype(BF16), preferred_element_type=F32)
    slot = lax.broadcasted_iota(jnp.int32, (slots, n_tok), 0)
    match = jnp.zeros((slots, n_tok), F32)
    weight = jnp.zeros((slots, n_tok), F32)
    for k in range(topk):
        position = jnp.sum(jnp.where(named[k], before, 0.0), axis=0, keepdims=True)
        here = slot == ids[k : k + 1, :] * cap + position.astype(jnp.int32)
        match = match + here.astype(F32)
        weight = weight + jnp.where(here, probs[k : k + 1, :], 0.0)
    weight = jnp.sum(weight, axis=1, keepdims=True)
    match = match.astype(BF16)
    match_ref[...] = match
    n_chunk = tok_ref.shape[1] // LANES
    for half, src in enumerate((tok_ref, grad_ref)):
        for c in range(0, n_chunk, 2):
            rows = jnp.dot(
                match, src[:, c * LANES : (c + 2) * LANES], preferred_element_type=F32
            )
            if half:
                rows = rows * weight
            for i in range(2):
                wide_ref[chunk_rows(half * n_chunk + c + i, slots, 2 * n_chunk), :] = rows[
                    :, i * LANES : (i + 1) * LANES
                ]
    out_ref[...] = wide_ref[...].astype(BF16)


def pack(ids, probs, tokens, out_grad, n_owner, cap):
    n_tok, width = tokens.shape
    slots = n_owner * cap
    rows = slots * 2 * width // LANES
    return pl.pallas_call(
        functools.partial(pack_kernel, cap),
        out_shape=(
            jax.ShapeDtypeStruct((rows, LANES), BF16),
            jax.ShapeDtypeStruct((slots, n_tok), BF16),
        ),
        scratch_shapes=[pltpu.VMEM((rows, LANES), F32)],
        name="pack",
    )(ids, probs, tokens, out_grad)


def near(value):
    return pltpu.with_memory_space_constraint(value, pltpu.VMEM)


def in_vmem():
    return pl.BlockSpec(memory_space=pltpu.VMEM)


def in_place():
    return pl.BlockSpec(memory_space=pl.ANY)


def fetch(where_ref, pieces, places, columns, into, sems, at):
    high, low = where_ref[0], where_ref[1]
    copies = []
    for i, (piece, (other, k, first)) in enumerate(zip(pieces, places)):
        block = jnp.bitwise_and(high + other, 1) * 4 + jnp.bitwise_and(low + 4 - k, 3)
        rows = pl.ds(pl.multiple_of(block * LANES + first, LANES // 2), piece.shape[0])
        copy = pltpu.make_async_copy(piece.at[:, columns], into.at[rows, :], sems.at[at + i])
        copy.start()
        copies.append(copy)
    return copies


def fetch_all(sources, targets, sems, at):
    copies = []
    for i, (source, target) in enumerate(zip(sources, targets)):
        copy = pltpu.make_async_copy(source, target, sems.at[at + i])
        copy.start()
        copies.append(copy)
    return copies


def slopes_kernel(pre_ref, act_ref, slope_ref, hid_ref):
    hidden = act_ref.shape[1]
    gate = pre_ref[:, :hidden].astype(F32)
    up = pre_ref[:, hidden:].astype(F32)
    sig = jax.nn.sigmoid(gate)
    act = gate * sig
    act_ref[...] = act
    slope_ref[...] = up * sig * (1.0 + gate * (1.0 - sig))
    hid_ref[...] = (act * up).astype(BF16)


def slopes(pre):
    slots, both = pre.shape
    hidden = both // 2
    return pl.pallas_call(
        slopes_kernel,
        out_shape=(
            jax.ShapeDtypeStruct((slots, hidden), F32),
            jax.ShapeDtypeStruct((slots, hidden), F32),
            jax.ShapeDtypeStruct((slots, hidden), BF16),
        ),
        name="slopes",
    )(pre)


def spread(wide_ref, first, step, into):
    slots, width = into.shape
    for c in range(width // LANES):
        into[:, c * LANES : (c + 1) * LANES] = wide_ref[
            chunk_rows(first + c, slots, step), :
        ].astype(BF16)


def core_kernel(places, *refs):
    n = len(places)
    where_ref, got_ref, act_hbm, slope_hbm, hid_hbm = refs[:5]
    pieces = refs[5 : 5 + n]
    row_hbm, part_refs = refs[5 + n], refs[6 + n : 10 + n]
    wide, x_rows, dy_rows, rows_wide, w1, w2, act, slope, hid, row, both, term, sems = refs[10 + n :]
    hidden = act.shape[1]
    slots, width = dy_rows.shape
    n_chunk = width // LANES
    first = fetch(where_ref, pieces, places, pl.ds(0, w1.shape[1]), w1, sems, 0)
    middle = fetch_all((slope_hbm, act_hbm), (slope, act), sems, 2 * n)
    last = fetch(where_ref, pieces, places, pl.ds(w1.shape[1], w2.shape[1]), w2, sems, n)
    last += fetch_all((hid_hbm,), (hid,), sems, 2 * n + 2)
    wide[...] = got_ref[...].astype(F32)
    spread(wide, n_chunk, 2 * n_chunk, dy_rows)
    spread(wide, 0, 2 * n_chunk, x_rows)
    for copy in first:
        copy.wait()
    grad = jnp.dot(dy_rows[...], w1[:, :hidden], preferred_element_type=F32)
    for copy in middle:
        copy.wait()
    both[:, :hidden] = (grad * slope[...]).astype(BF16)
    both[:, hidden:] = (grad * act[...]).astype(BF16)
    for copy in last:
        copy.wait()
    for c in range(0, n_chunk, 2):
        rows = lax.dot_general(
            both[...],
            w2[c * LANES : (c + 2) * LANES, :],
            (((1,), (1,)), ((), ())),
            preferred_element_type=F32,
        )
        rows_wide[chunk_rows(c, slots, n_chunk), :] = rows[:, :LANES]
        rows_wide[chunk_rows(c + 1, slots, n_chunk), :] = rows[:, LANES:]
    row[...] = rows_wide[...].astype(BF16)
    sent = fetch_all((row,), (row_hbm,), sems, 2 * n + 3)
    x_proj = jnp.dot(x_rows[...], w1[:, hidden:], preferred_element_type=F32).astype(BF16)
    dy_proj = jnp.dot(dy_rows[...], w1[:, hidden:], preferred_element_type=F32).astype(BF16)
    by_rows = (((0,), (0,)), ((), ()))
    for t, (left, right) in enumerate(
        ((x_proj, both[:, :hidden]), (x_proj, both[:, hidden:]), (dy_proj, hid[...]))
    ):
        term[t] = lax.dot_general(left, right, by_rows, preferred_element_type=F32).astype(BF16)
    high, low = where_ref[0], where_ref[1]
    part = part_refs[0].shape[2]
    for k, out in enumerate(part_refs):
        column = jnp.bitwise_and(low + k, 3)
        for h in range(2):
            begin = (jnp.bitwise_and(high + h, 1) * 4 + column) * part
            rows = term.at[:, pl.ds(pl.multiple_of(begin, part), part), :]
            sent += fetch_all((rows,), (out.at[h],), sems, 2 * n + 4 + 2 * k + h)
    for copy in sent:
        copy.wait()


def core(where, got, act, slope, hid, pieces, places, rank, n_dp):
    slots, hidden = act.shape
    width = got.shape[0] * LANES // slots // 2
    rows = slots * width // LANES
    part = rank // n_dp
    n = len(pieces)
    return pl.pallas_call(
        functools.partial(core_kernel, places),
        in_specs=[pl.BlockSpec(memory_space=pltpu.SMEM), in_vmem()] + [in_place()] * (3 + n),
        out_specs=(in_place(),) * 5,
        out_shape=(
            jax.ShapeDtypeStruct((rows, LANES), BF16),
            *(jax.ShapeDtypeStruct((2, 3, part, hidden), BF16) for _ in range(4)),
        ),
        scratch_shapes=[
            pltpu.VMEM(got.shape, F32),
            pltpu.VMEM((slots, width), BF16),
            pltpu.VMEM((slots, width), BF16),
            pltpu.VMEM((rows, LANES), F32),
            pltpu.VMEM((width, hidden + rank), BF16),
            pltpu.VMEM((width, 2 * hidden), BF16),
            pltpu.VMEM((slots, hidden), F32),
            pltpu.VMEM((slots, hidden), F32),
            pltpu.VMEM((slots, hidden), BF16),
            pltpu.VMEM((rows, LANES), BF16),
            pltpu.VMEM((slots, 2 * hidden), BF16),
            pltpu.VMEM((3, rank, hidden), BF16),
            pltpu.SemaphoreType.DMA((2 * n + 12,)),
        ],
        name="core",
    )(where, near(got), act, slope, hid, *pieces)


def take_pair(wide_ref, first, second, slots, step):
    return jnp.concatenate(
        [
            wide_ref[chunk_rows(first, slots, step), :],
            wide_ref[chunk_rows(second, slots, step), :],
        ],
        axis=1,
    ).astype(BF16)


def combine_kernel(match_ref, got_ref, out_ref, wide_ref):
    slots = match_ref.shape[0]
    n_chunk = out_ref.shape[1] // LANES
    wide_ref[...] = got_ref[...].astype(F32)
    for c in range(0, n_chunk, 2):
        rows = take_pair(wide_ref, c, c + 1, slots, n_chunk)
        total = lax.dot_general(
            match_ref[...], rows, (((0,), (0,)), ((), ())), preferred_element_type=F32
        )
        out_ref[:, c * LANES : (c + 2) * LANES] = total.astype(BF16)


def combine(match, got, width):
    n_tok = match.shape[1]
    return pl.pallas_call(
        combine_kernel,
        out_shape=jax.ShapeDtypeStruct((n_tok, width), BF16),
        scratch_shapes=[pltpu.VMEM(got.shape, F32)],
        name="combine",
    )(match, near(got))


def swap(value):
    return lax.ppermute(value, "dp_0", [(0, 1), (1, 0)])


def shifted(value, k):
    size = lax.axis_size("dp_1")
    return lax.ppermute(value, "dp_1", [(i, (i + k) % size) for i in range(size)])


def exchange(value, n_owner):
    rows, lanes = value.shape
    out = lax.all_to_all(
        value.reshape(n_owner, rows // n_owner, lanes), "expert", 0, 0, tiled=True
    )
    return out.reshape(rows, lanes)


def body(
    tokens, out_grad, expert_ids, gate_probs, saved_pre, gate_weight, up_weight, down_weight, basis
):
    n_owner = lax.axis_size("expert")
    width = tokens.shape[1]
    slots = saved_pre.shape[2]
    cap = slots // n_owner
    where = jnp.stack([lax.axis_index("dp_0"), lax.axis_index("dp_1")]).astype(jnp.int32)

    own = jnp.concatenate([down_weight[0], basis[0], gate_weight[0], up_weight[0]], axis=1)
    far = swap(own)
    sent, match = pack(expert_ids.T, gate_probs.T, tokens, out_grad, n_owner, cap)
    got = exchange(sent, n_owner)
    pieces, places = [], []
    half = own.shape[0] // 2
    for other, block in enumerate((own, far)):
        left, right = shifted(block, 1), shifted(block, -1)
        top, bottom = shifted(left[:half], 1), shifted(right[half:], -1)
        pieces += [block, left, right, top, bottom]
        places += [(other, 0, 0), (other, 1, 0), (other, 3, 0), (other, 2, 0), (other, 2, half)]
    rank = basis.shape[2]
    act, slope, hid = slopes(saved_pre[0, 0])
    places = tuple(places)
    row_grad, *parts = core(where, got, act, slope, hid, pieces, places, rank, 8)
    back = exchange(row_grad, n_owner)
    summed = parts[0].astype(F32)
    for k in (2, 1, 3):
        summed = summed + shifted(parts[k], k).astype(F32)
    other = swap(summed[1].astype(BF16))
    proj_grads = (summed[0] + other.astype(F32))[None]
    in_grad = combine(match, back, width)
    return in_grad, proj_grads


def solution(mesh):
    finer = Mesh(mesh.devices.reshape(2, 4, mesh.shape["expert"]), DP_EXPERT)
    placed = (
        P(DP_EXPERT, None),
        P(DP_EXPERT, None),
        P(DP_EXPERT, None),
        P(DP_EXPERT, None),
        P(DP, "expert", None, None),
        P("expert", DP, None),
        P("expert", DP, None),
        P("expert", DP, None),
        P("expert", DP, None),
    )
    return jax.shard_map(
        body,
        mesh=finer,
        in_specs=placed,
        out_specs=(P(DP_EXPERT, None), P("expert", None, DP, None)),
        check_vma=False,
    )
```

```python
import functools

import jax
import jax.numpy as jnp
from jax import lax
from jax.experimental import pallas as pl
from jax.experimental.pallas import tpu as pltpu
from jax.sharding import Mesh
from jax.sharding import PartitionSpec as P


DP = ("dp_0", "dp_1")
DP_EXPERT = ("dp_0", "dp_1", "expert")
F32 = jnp.float32
BF16 = jnp.bfloat16
LANES = 128


def chunk_rows(start, slots, step):
    return pl.ds(start, slots, stride=step)


def pack_kernel(cap, ids_ref, probs_ref, tok_ref, grad_ref, out_ref, match_ref, wide_ref):
    slots, n_tok = match_ref.shape
    topk = ids_ref.shape[0]
    n_owner = slots // cap
    ids = ids_ref[...]
    probs = probs_ref[...]
    owner = lax.broadcasted_iota(jnp.int32, (n_owner, n_tok), 0)
    named = [owner == ids[k : k + 1, :] for k in range(topk)]
    per_owner = sum(n.astype(F32) for n in named)
    earlier = (
        lax.broadcasted_iota(jnp.int32, (n_tok, n_tok), 0)
        < lax.broadcasted_iota(jnp.int32, (n_tok, n_tok), 1)
    ).astype(F32)
    before = jnp.dot(per_owner.astype(BF16), earlier.astype(BF16), preferred_element_type=F32)
    slot = lax.broadcasted_iota(jnp.int32, (slots, n_tok), 0)
    match = jnp.zeros((slots, n_tok), F32)
    weight = jnp.zeros((slots, n_tok), F32)
    for k in range(topk):
        position = jnp.sum(jnp.where(named[k], before, 0.0), axis=0, keepdims=True)
        here = slot == ids[k : k + 1, :] * cap + position.astype(jnp.int32)
        match = match + here.astype(F32)
        weight = weight + jnp.where(here, probs[k : k + 1, :], 0.0)
    weight = jnp.sum(weight, axis=1, keepdims=True)
    match = match.astype(BF16)
    match_ref[...] = match
    n_chunk = tok_ref.shape[1] // LANES
    for half, src in enumerate((tok_ref, grad_ref)):
        for c in range(0, n_chunk, 2):
            rows = jnp.dot(
                match, src[:, c * LANES : (c + 2) * LANES], preferred_element_type=F32
            )
            if half:
                rows = rows * weight
            for i in range(2):
                wide_ref[chunk_rows(half * n_chunk + c + i, slots, 2 * n_chunk), :] = rows[
                    :, i * LANES : (i + 1) * LANES
                ]
    out_ref[...] = wide_ref[...].astype(BF16)


def pack(ids, probs, tokens, out_grad, n_owner, cap):
    n_tok, width = tokens.shape
    slots = n_owner * cap
    rows = slots * 2 * width // LANES
    return pl.pallas_call(
        functools.partial(pack_kernel, cap),
        out_shape=(
            jax.ShapeDtypeStruct((rows, LANES), BF16),
            jax.ShapeDtypeStruct((slots, n_tok), BF16),
        ),
        scratch_shapes=[pltpu.VMEM((rows, LANES), F32)],
        name="pack",
    )(ids, probs, tokens, out_grad)


def near(value):
    return pltpu.with_memory_space_constraint(value, pltpu.VMEM)


def in_vmem():
    return pl.BlockSpec(memory_space=pltpu.VMEM)


def in_place():
    return pl.BlockSpec(memory_space=pl.ANY)


def fetch(where_ref, pieces, places, columns, into, sems, at):
    high, low = where_ref[0], where_ref[1]
    copies = []
    for i, (piece, (other, k, first)) in enumerate(zip(pieces, places)):
        block = jnp.bitwise_and(high + other, 1) * 4 + jnp.bitwise_and(low + 4 - k, 3)
        rows = pl.ds(pl.multiple_of(block * LANES + first, LANES // 2), piece.shape[0])
        copy = pltpu.make_async_copy(piece.at[:, columns], into.at[rows, :], sems.at[at + i])
        copy.start()
        copies.append(copy)
    return copies


def fetch_all(sources, targets, sems, at):
    copies = []
    for i, (source, target) in enumerate(zip(sources, targets)):
        copy = pltpu.make_async_copy(source, target, sems.at[at + i])
        copy.start()
        copies.append(copy)
    return copies


def slopes_kernel(pre_ref, act_ref, slope_ref, hid_ref):
    hidden = act_ref.shape[1]
    gate = pre_ref[:, :hidden].astype(F32)
    up = pre_ref[:, hidden:].astype(F32)
    sig = jax.nn.sigmoid(gate)
    act = gate * sig
    act_ref[...] = act
    slope_ref[...] = up * sig * (1.0 + gate * (1.0 - sig))
    hid_ref[...] = (act * up).astype(BF16)


def slopes(pre):
    slots, both = pre.shape
    hidden = both // 2
    return pl.pallas_call(
        slopes_kernel,
        out_shape=(
            jax.ShapeDtypeStruct((slots, hidden), F32),
            jax.ShapeDtypeStruct((slots, hidden), F32),
            jax.ShapeDtypeStruct((slots, hidden), BF16),
        ),
        name="slopes",
    )(pre)


def core_kernel(places, *refs):
    n = len(places)
    where_ref, got_ref, act_hbm, slope_hbm, hid_hbm = refs[:5]
    pieces = refs[5 : 5 + n]
    row_hbm, part_refs = refs[5 + n], refs[6 + n : 10 + n]
    _, x_rows, dy_rows, rows_wide, w1, w2, act, slope, hid, row, both, term, sems = refs[10 + n :]
    hidden = act.shape[1]
    rank = w1.shape[1] - hidden
    slots, width = dy_rows.shape
    n_chunk = width // LANES
    down_in = fetch(where_ref, pieces, places, pl.ds(0, hidden), w1.at[:, pl.ds(0, hidden)], sems, 0)
    factors_in = fetch_all((slope_hbm, act_hbm), (slope, act), sems, 3 * n)
    tiles = got_ref[...].reshape(slots, 2 * n_chunk, LANES)
    dy_rows[...] = tiles[:, n_chunk:, :].reshape(slots, width)
    x_rows[...] = tiles[:, :n_chunk, :].reshape(slots, width)
    for copy in down_in:
        copy.wait()
    basis_in = fetch(
        where_ref, pieces, places, pl.ds(hidden, rank), w1.at[:, pl.ds(hidden, rank)], sems, n
    )
    basis_in += fetch_all((hid_hbm,), (hid,), sems, 3 * n + 2)
    w2_in = fetch(
        where_ref, pieces, places, pl.ds(hidden + rank, w2.shape[1]), w2, sems, 2 * n
    )
    grad = jnp.dot(dy_rows[...], w1[:, :hidden], preferred_element_type=F32)
    for copy in factors_in:
        copy.wait()
    both[:, :hidden] = (grad * slope[...]).astype(BF16)
    both[:, hidden:] = (grad * act[...]).astype(BF16)
    for copy in basis_in:
        copy.wait()
    dy_proj = jnp.dot(dy_rows[...], w1[:, hidden:], preferred_element_type=F32).astype(BF16)
    x_proj = jnp.dot(x_rows[...], w1[:, hidden:], preferred_element_type=F32).astype(BF16)
    by_rows = (((0,), (0,)), ((), ()))
    for t, (left, right) in enumerate(
        ((x_proj, both[:, :hidden]), (x_proj, both[:, hidden:]), (dy_proj, hid[...]))
    ):
        term[t] = lax.dot_general(left, right, by_rows, preferred_element_type=F32).astype(BF16)
    high, low = where_ref[0], where_ref[1]
    part = part_refs[0].shape[2]
    sent = []
    for k, out in enumerate(part_refs):
        column = jnp.bitwise_and(low + k, 3)
        for h in range(2):
            begin = (jnp.bitwise_and(high + h, 1) * 4 + column) * part
            rows = term.at[:, pl.ds(pl.multiple_of(begin, part), part), :]
            sent += fetch_all((rows,), (out.at[h],), sems, 3 * n + 3 + 2 * k + h)
    for copy in w2_in:
        copy.wait()
    for c in range(0, n_chunk, 2):
        rows = lax.dot_general(
            both[...],
            w2[c * LANES : (c + 2) * LANES, :],
            (((1,), (1,)), ((), ())),
            preferred_element_type=F32,
        )
        rows_wide[chunk_rows(c, slots, n_chunk), :] = rows[:, :LANES]
        rows_wide[chunk_rows(c + 1, slots, n_chunk), :] = rows[:, LANES:]
    size = row.shape[0] // 4
    for i in range(4):
        here = pl.ds(i * size, size)
        row[here, :] = rows_wide[here, :].astype(BF16)
        sent += fetch_all((row.at[here, :],), (row_hbm.at[here, :],), sems, 3 * n + 11 + i)
    for copy in sent:
        copy.wait()


def core(where, got, act, slope, hid, pieces, places, rank, n_dp):
    slots, hidden = act.shape
    width = got.shape[0] * LANES // slots // 2
    rows = slots * width // LANES
    part = rank // n_dp
    n = len(pieces)
    return pl.pallas_call(
        functools.partial(core_kernel, places),
        in_specs=[pl.BlockSpec(memory_space=pltpu.SMEM), in_vmem()] + [in_place()] * (3 + n),
        out_specs=(in_place(),) * 5,
        out_shape=(
            jax.ShapeDtypeStruct((rows, LANES), BF16),
            *(jax.ShapeDtypeStruct((2, 3, part, hidden), BF16) for _ in range(4)),
        ),
        scratch_shapes=[
            pltpu.VMEM(got.shape, F32),
            pltpu.VMEM((slots, width), BF16),
            pltpu.VMEM((slots, width), BF16),
            pltpu.VMEM((rows, LANES), F32),
            pltpu.VMEM((width, hidden + rank), BF16),
            pltpu.VMEM((width, 2 * hidden), BF16),
            pltpu.VMEM((slots, hidden), F32),
            pltpu.VMEM((slots, hidden), F32),
            pltpu.VMEM((slots, hidden), BF16),
            pltpu.VMEM((rows, LANES), BF16),
            pltpu.VMEM((slots, 2 * hidden), BF16),
            pltpu.VMEM((3, rank, hidden), BF16),
            pltpu.SemaphoreType.DMA((3 * n + 15,)),
        ],
        name="core",
    )(where, near(got), act, slope, hid, *pieces)


def take_pair(wide_ref, first, second, slots, step):
    return jnp.concatenate(
        [
            wide_ref[chunk_rows(first, slots, step), :],
            wide_ref[chunk_rows(second, slots, step), :],
        ],
        axis=1,
    ).astype(BF16)


def combine_kernel(match_ref, got_ref, out_ref, wide_ref):
    slots = match_ref.shape[0]
    n_chunk = out_ref.shape[1] // LANES
    wide_ref[...] = got_ref[...].astype(F32)
    for c in range(0, n_chunk, 2):
        rows = take_pair(wide_ref, c, c + 1, slots, n_chunk)
        total = lax.dot_general(
            match_ref[...], rows, (((0,), (0,)), ((), ())), preferred_element_type=F32
        )
        out_ref[:, c * LANES : (c + 2) * LANES] = total.astype(BF16)


def combine(match, got, width):
    n_tok = match.shape[1]
    return pl.pallas_call(
        combine_kernel,
        out_shape=jax.ShapeDtypeStruct((n_tok, width), BF16),
        scratch_shapes=[pltpu.VMEM(got.shape, F32)],
        name="combine",
    )(near(match), near(got))


def swap(value):
    return lax.ppermute(value, "dp_0", [(0, 1), (1, 0)])


def shifted(value, k):
    size = lax.axis_size("dp_1")
    return lax.ppermute(value, "dp_1", [(i, (i + k) % size) for i in range(size)])


def exchange(value, n_owner):
    rows, lanes = value.shape
    out = lax.all_to_all(
        value.reshape(n_owner, rows // n_owner, lanes), "expert", 0, 0, tiled=True
    )
    return out.reshape(rows, lanes)


def body(
    tokens, out_grad, expert_ids, gate_probs, saved_pre, gate_weight, up_weight, down_weight, basis
):
    n_owner = lax.axis_size("expert")
    width = tokens.shape[1]
    slots = saved_pre.shape[2]
    cap = slots // n_owner
    where = jnp.stack([lax.axis_index("dp_0"), lax.axis_index("dp_1")]).astype(jnp.int32)

    own = jnp.concatenate([down_weight[0], basis[0], gate_weight[0], up_weight[0]], axis=1)
    far = swap(own)
    sent, match = pack(expert_ids.T, gate_probs.T, tokens, out_grad, n_owner, cap)
    got = exchange(sent, n_owner)
    pieces, places = [], []
    half = own.shape[0] // 2
    for other, block in enumerate((own, far)):
        left, right = shifted(block, 1), shifted(block, -1)
        top, bottom = shifted(left[:half], 1), shifted(right[half:], -1)
        pieces += [block, left, right, top, bottom]
        places += [(other, 0, 0), (other, 1, 0), (other, 3, 0), (other, 2, 0), (other, 2, half)]
    rank = basis.shape[2]
    act, slope, hid = slopes(saved_pre[0, 0])
    places = tuple(places)
    row_grad, *parts = core(where, got, act, slope, hid, pieces, places, rank, 8)
    back = exchange(row_grad, n_owner)
    summed = parts[0].astype(F32)
    for k in (2, 1, 3):
        summed = summed + shifted(parts[k], k).astype(F32)
    other = swap(summed[1].astype(BF16))
    proj_grads = (summed[0] + other.astype(F32))[None]
    in_grad = combine(match, back, width)
    return in_grad, proj_grads


def solution(mesh):
    finer = Mesh(mesh.devices.reshape(2, 4, mesh.shape["expert"]), DP_EXPERT)
    placed = (
        P(DP_EXPERT, None),
        P(DP_EXPERT, None),
        P(DP_EXPERT, None),
        P(DP_EXPERT, None),
        P(DP, "expert", None, None),
        P("expert", DP, None),
        P("expert", DP, None),
        P("expert", DP, None),
        P("expert", DP, None),
    )
    return jax.shard_map(
        body,
        mesh=finer,
        in_specs=placed,
        out_specs=(P(DP_EXPERT, None), P("expert", None, DP, None)),
        check_vma=False,
    )
```

```python
import functools

import jax
import jax.numpy as jnp
from jax import lax
from jax.experimental import pallas as pl
from jax.experimental.pallas import tpu as pltpu
from jax.sharding import Mesh
from jax.sharding import PartitionSpec as P


DP = ("dp_0", "dp_1")
DP_EXPERT = ("dp_0", "dp_1", "expert")
F32 = jnp.float32
BF16 = jnp.bfloat16
LANES = 128


def chunk_rows(start, slots, step):
    return pl.ds(start, slots, stride=step)


def pack_kernel(cap, ids_ref, probs_ref, tok_ref, grad_ref, out_ref, match_ref, wide_ref):
    slots, n_tok = match_ref.shape
    topk = ids_ref.shape[0]
    n_owner = slots // cap
    ids = ids_ref[...]
    probs = probs_ref[...]
    owner = lax.broadcasted_iota(jnp.int32, (n_owner, n_tok), 0)
    named = [owner == ids[k : k + 1, :] for k in range(topk)]
    per_owner = sum(n.astype(F32) for n in named)
    earlier = (
        lax.broadcasted_iota(jnp.int32, (n_tok, n_tok), 0)
        < lax.broadcasted_iota(jnp.int32, (n_tok, n_tok), 1)
    ).astype(F32)
    before = jnp.dot(per_owner.astype(BF16), earlier.astype(BF16), preferred_element_type=F32)
    slot = lax.broadcasted_iota(jnp.int32, (slots, n_tok), 0)
    match = jnp.zeros((slots, n_tok), F32)
    weight = jnp.zeros((slots, n_tok), F32)
    for k in range(topk):
        position = jnp.sum(jnp.where(named[k], before, 0.0), axis=0, keepdims=True)
        here = slot == ids[k : k + 1, :] * cap + position.astype(jnp.int32)
        match = match + here.astype(F32)
        weight = weight + jnp.where(here, probs[k : k + 1, :], 0.0)
    weight = jnp.sum(weight, axis=1, keepdims=True)
    match = match.astype(BF16)
    match_ref[...] = match
    n_chunk = tok_ref.shape[1] // LANES
    for half, src in enumerate((tok_ref, grad_ref)):
        for c in range(0, n_chunk, 2):
            rows = jnp.dot(
                match, src[:, c * LANES : (c + 2) * LANES], preferred_element_type=F32
            )
            if half:
                rows = rows * weight
            for i in range(2):
                wide_ref[chunk_rows(half * n_chunk + c + i, slots, 2 * n_chunk), :] = rows[
                    :, i * LANES : (i + 1) * LANES
                ]
    out_ref[...] = wide_ref[...].astype(BF16)


def pack(ids, probs, tokens, out_grad, n_owner, cap):
    n_tok, width = tokens.shape
    slots = n_owner * cap
    rows = slots * 2 * width // LANES
    return pl.pallas_call(
        functools.partial(pack_kernel, cap),
        out_shape=(
            jax.ShapeDtypeStruct((rows, LANES), BF16),
            jax.ShapeDtypeStruct((slots, n_tok), BF16),
        ),
        scratch_shapes=[pltpu.VMEM((rows, LANES), F32)],
        name="pack",
    )(ids, probs, tokens, out_grad)


def near(value):
    return pltpu.with_memory_space_constraint(value, pltpu.VMEM)


def in_vmem():
    return pl.BlockSpec(memory_space=pltpu.VMEM)


def in_place():
    return pl.BlockSpec(memory_space=pl.ANY)


def fetch(where_ref, pieces, places, columns, into, sems, at):
    high, low = where_ref[0], where_ref[1]
    copies = []
    for i, (piece, (other, k, first)) in enumerate(zip(pieces, places)):
        block = jnp.bitwise_and(high + other, 1) * 4 + jnp.bitwise_and(low + 4 - k, 3)
        rows = pl.ds(pl.multiple_of(block * LANES + first, LANES // 2), piece.shape[0])
        copy = pltpu.make_async_copy(piece.at[:, columns], into.at[rows, :], sems.at[at + i])
        copy.start()
        copies.append(copy)
    return copies


def fetch_all(sources, targets, sems, at):
    copies = []
    for i, (source, target) in enumerate(zip(sources, targets)):
        copy = pltpu.make_async_copy(source, target, sems.at[at + i])
        copy.start()
        copies.append(copy)
    return copies


def slopes_kernel(pre_ref, act_ref, slope_ref, hid_ref):
    hidden = act_ref.shape[1]
    gate = pre_ref[:, :hidden].astype(F32)
    up = pre_ref[:, hidden:].astype(F32)
    sig = jax.nn.sigmoid(gate)
    act = gate * sig
    act_ref[...] = act
    slope_ref[...] = up * sig * (1.0 + gate * (1.0 - sig))
    hid_ref[...] = (act * up).astype(BF16)


def slopes(pre):
    slots, both = pre.shape
    hidden = both // 2
    return pl.pallas_call(
        slopes_kernel,
        out_shape=(
            jax.ShapeDtypeStruct((slots, hidden), F32),
            jax.ShapeDtypeStruct((slots, hidden), F32),
            jax.ShapeDtypeStruct((slots, hidden), BF16),
        ),
        name="slopes",
    )(pre)


def core_kernel(places, *refs):
    n = len(places)
    where_ref, got_ref, act_hbm, slope_hbm, hid_hbm = refs[:5]
    pieces = refs[5 : 5 + n]
    row_hbm, part_refs = refs[5 + n], refs[6 + n : 10 + n]
    _, x_rows, dy_rows, rows_wide, w1, w2, act, slope, hid, row, both, term, sems = refs[10 + n :]
    hidden = act.shape[1]
    rank = w1.shape[1] - hidden
    slots, width = dy_rows.shape
    n_chunk = width // LANES
    down_in = fetch(where_ref, pieces, places, pl.ds(0, hidden), w1.at[:, pl.ds(0, hidden)], sems, 0)
    factors_in = fetch_all((slope_hbm, act_hbm), (slope, act), sems, 3 * n)
    tiles = got_ref[...].reshape(slots, 2 * n_chunk, LANES)
    dy_rows[...] = tiles[:, n_chunk:, :].reshape(slots, width)
    x_rows[...] = tiles[:, :n_chunk, :].reshape(slots, width)
    for copy in down_in:
        copy.wait()
    basis_in = fetch(
        where_ref, pieces, places, pl.ds(hidden, rank), w1.at[:, pl.ds(hidden, rank)], sems, n
    )
    basis_in += fetch_all((hid_hbm,), (hid,), sems, 3 * n + 2)
    w2_in = fetch(
        where_ref, pieces, places, pl.ds(hidden + rank, w2.shape[1]), w2, sems, 2 * n
    )
    grad = jnp.dot(dy_rows[...], w1[:, :hidden], preferred_element_type=F32)
    for copy in factors_in:
        copy.wait()
    both[:, :hidden] = (grad * act[...]).astype(BF16)
    both[:, hidden:] = (grad * slope[...]).astype(BF16)
    for copy in basis_in:
        copy.wait()
    dy_proj = jnp.dot(dy_rows[...], w1[:, hidden:], preferred_element_type=F32).astype(BF16)
    x_proj = jnp.dot(x_rows[...], w1[:, hidden:], preferred_element_type=F32).astype(BF16)
    by_rows = (((0,), (0,)), ((), ()))
    for t, (left, right) in enumerate(
        ((x_proj, both[:, hidden:]), (x_proj, both[:, :hidden]), (dy_proj, hid[...]))
    ):
        term[t] = lax.dot_general(left, right, by_rows, preferred_element_type=F32).astype(BF16)
    high, low = where_ref[0], where_ref[1]
    part = part_refs[0].shape[2]
    sent = []
    for k, out in enumerate(part_refs):
        column = jnp.bitwise_and(low + k, 3)
        for h in range(2):
            begin = (jnp.bitwise_and(high + h, 1) * 4 + column) * part
            rows = term.at[:, pl.ds(pl.multiple_of(begin, part), part), :]
            sent += fetch_all((rows,), (out.at[h],), sems, 3 * n + 3 + 2 * k + h)
    for copy in w2_in:
        copy.wait()
    for c in range(0, n_chunk, 2):
        rows = lax.dot_general(
            both[...],
            w2[c * LANES : (c + 2) * LANES, :],
            (((1,), (1,)), ((), ())),
            preferred_element_type=F32,
        )
        rows_wide[chunk_rows(c, slots, n_chunk), :] = rows[:, :LANES]
        rows_wide[chunk_rows(c + 1, slots, n_chunk), :] = rows[:, LANES:]
    size = row.shape[0] // 4
    for i in range(4):
        here = pl.ds(i * size, size)
        row[here, :] = rows_wide[here, :].astype(BF16)
        sent += fetch_all((row.at[here, :],), (row_hbm.at[here, :],), sems, 3 * n + 11 + i)
    for copy in sent:
        copy.wait()


def core(where, got, act, slope, hid, pieces, places, rank, n_dp):
    slots, hidden = act.shape
    width = got.shape[0] * LANES // slots // 2
    rows = slots * width // LANES
    part = rank // n_dp
    n = len(pieces)
    return pl.pallas_call(
        functools.partial(core_kernel, places),
        in_specs=[pl.BlockSpec(memory_space=pltpu.SMEM), in_vmem()] + [in_place()] * (3 + n),
        out_specs=(in_place(),) * 5,
        out_shape=(
            jax.ShapeDtypeStruct((rows, LANES), BF16),
            *(jax.ShapeDtypeStruct((2, 3, part, hidden), BF16) for _ in range(4)),
        ),
        scratch_shapes=[
            pltpu.VMEM(got.shape, F32),
            pltpu.VMEM((slots, width), BF16),
            pltpu.VMEM((slots, width), BF16),
            pltpu.VMEM((rows, LANES), F32),
            pltpu.VMEM((width, hidden + rank), BF16),
            pltpu.VMEM((width, 2 * hidden), BF16),
            pltpu.VMEM((slots, hidden), F32),
            pltpu.VMEM((slots, hidden), F32),
            pltpu.VMEM((slots, hidden), BF16),
            pltpu.VMEM((rows, LANES), BF16),
            pltpu.VMEM((slots, 2 * hidden), BF16),
            pltpu.VMEM((3, rank, hidden), BF16),
            pltpu.SemaphoreType.DMA((3 * n + 15,)),
        ],
        name="core",
    )(where, near(got), act, slope, hid, *pieces)


def take_pair(wide_ref, first, second, slots, step):
    return jnp.concatenate(
        [
            wide_ref[chunk_rows(first, slots, step), :],
            wide_ref[chunk_rows(second, slots, step), :],
        ],
        axis=1,
    ).astype(BF16)


def combine_kernel(match_ref, got_ref, out_ref, wide_ref):
    slots = match_ref.shape[0]
    n_chunk = out_ref.shape[1] // LANES
    wide_ref[...] = got_ref[...].astype(F32)
    for c in range(0, n_chunk, 2):
        rows = take_pair(wide_ref, c, c + 1, slots, n_chunk)
        total = lax.dot_general(
            match_ref[...], rows, (((0,), (0,)), ((), ())), preferred_element_type=F32
        )
        out_ref[:, c * LANES : (c + 2) * LANES] = total.astype(BF16)


def combine(match, got, width):
    n_tok = match.shape[1]
    return pl.pallas_call(
        combine_kernel,
        out_shape=jax.ShapeDtypeStruct((n_tok, width), BF16),
        scratch_shapes=[pltpu.VMEM(got.shape, F32)],
        name="combine",
    )(near(match), near(got))


def swap(value):
    return lax.ppermute(value, "dp_0", [(0, 1), (1, 0)])


def shifted(value, k):
    size = lax.axis_size("dp_1")
    return lax.ppermute(value, "dp_1", [(i, (i + k) % size) for i in range(size)])


def exchange(value, n_owner):
    rows, lanes = value.shape
    out = lax.all_to_all(
        value.reshape(n_owner, rows // n_owner, lanes), "expert", 0, 0, tiled=True
    )
    return out.reshape(rows, lanes)


def body(
    tokens, out_grad, expert_ids, gate_probs, saved_pre, gate_weight, up_weight, down_weight, basis
):
    n_owner = lax.axis_size("expert")
    width = tokens.shape[1]
    slots = saved_pre.shape[2]
    cap = slots // n_owner
    where = jnp.stack([lax.axis_index("dp_0"), lax.axis_index("dp_1")]).astype(jnp.int32)

    far_gate = swap(gate_weight[0])
    rest = jnp.concatenate([down_weight[0], basis[0], up_weight[0]], axis=1)
    far_rest = swap(rest)
    sent, match = pack(expert_ids.T, gate_probs.T, tokens, out_grad, n_owner, cap)
    got = exchange(sent, n_owner)
    own = jnp.concatenate([rest, gate_weight[0]], axis=1)
    far = jnp.concatenate([far_rest, far_gate], axis=1)
    pieces, places = [], []
    half = own.shape[0] // 2
    for other, block in enumerate((own, far)):
        left, right = shifted(block, 1), shifted(block, -1)
        top, bottom = shifted(left[:half], 1), shifted(right[half:], -1)
        pieces += [block, left, right, top, bottom]
        places += [(other, 0, 0), (other, 1, 0), (other, 3, 0), (other, 2, 0), (other, 2, half)]
    rank = basis.shape[2]
    act, slope, hid = slopes(saved_pre[0, 0])
    places = tuple(places)
    row_grad, *parts = core(where, got, act, slope, hid, pieces, places, rank, 8)
    back = exchange(row_grad, n_owner)
    summed = parts[0].astype(F32)
    for k in (2, 1, 3):
        summed = summed + shifted(parts[k], k).astype(F32)
    other = swap(summed[1].astype(BF16))
    proj_grads = (summed[0] + other.astype(F32))[None]
    in_grad = combine(match, back, width)
    return in_grad, proj_grads


def solution(mesh):
    finer = Mesh(mesh.devices.reshape(2, 4, mesh.shape["expert"]), DP_EXPERT)
    placed = (
        P(DP_EXPERT, None),
        P(DP_EXPERT, None),
        P(DP_EXPERT, None),
        P(DP_EXPERT, None),
        P(DP, "expert", None, None),
        P("expert", DP, None),
        P("expert", DP, None),
        P("expert", DP, None),
        P("expert", DP, None),
    )
    return jax.shard_map(
        body,
        mesh=finer,
        in_specs=placed,
        out_specs=(P(DP_EXPERT, None), P("expert", None, DP, None)),
        check_vma=False,
    )
```
